128 devices in a mesh: ep: 32 (over z, x, core), dp: 4 (over y).
Axes of the slice: x: 4, y: 4, z: 4, core: 2. Of those that a mesh axis runs over, the one named last changes fastest.
Arguments:
- residual: bfloat16 [16384, 2880], P(('ep', 'dp')), may hold values from -400 to 400, as said below
- norm_gain: float32 [2880], replicated, may hold values from 0.25 to 1.75
- router_weight: bfloat16 [2880, 128], replicated, may hold values from -0.109375 to 0.109375
- out_grad: bfloat16 [16384, 2880], P(('ep', 'dp')), may hold values from -6 to 6
- expert_ids: int32 [16384, 4], P(('ep', 'dp')), may hold values from 0 to 127, all different within a row; in each aligned block of 128 rows (0 to 127, 128 to 255, ...) at most 6 rows name the same one
- hidden: bfloat16 [128, 768, 1440], P(('ep', 'dp')), may hold values from -0.3125 to 0.3125
- down_weight: bfloat16 [128, 1440, 2880], P(('ep', 'dp')), may hold values from -0.15625 to 0.15625
Outputs:
- hidden_grad: bfloat16 [128, 768, 1440], P(('ep', 'dp'))
- down_weight_grad: bfloat16 [128, 1440, 2880], P(('ep', 'dp'))
- residual_grad: bfloat16 [16384, 2880], P(('ep', 'dp'))
- router_grad: float32 [2880, 128], replicated
- gain_grad: float32 [2880], replicated
The draws below stay inside these ranges and needn't reach their ends.
Inputs may be any that keep to these rules, and one draw needn't show every extreme that they name: `expert_ids`: in the tokens of one device no expert is named more than 6 times, a bound that some block reaches. `residual`: Real-valued entries.
All inputs are finite; a program needn't handle non-finite values.
Results may differ from the reference program's by a relative error of at most 0.0085.
Values may be sent and summed in bfloat16 or wider, within the bound.
A program may use at most 128 MiB of HBM per device.

```python
import math
import jax
import jax.numpy as jnp
import numpy as np
from jax import lax

D = 2880
TOPK = 4
FF = 1440
TOK_DEV = 128
EXPERTS = 128
TOKENS = 16384
CAP = 6
SLOTS = 768
N_EP = 32
N_DP = 4


def draw_residual(key, part):
    key_rows, key_cols, key_base = jax.random.split(key, 3)
    row_scale = jnp.exp(jax.random.uniform(key_rows, (TOKENS, 1), jnp.float32, 0.0, math.log(10.0)))
    column_scale = jnp.exp(jax.random.uniform(key_cols, (1, D), jnp.float32, 0.0, math.log(10.0)))
    base = jax.random.truncated_normal(key_base, -3.5, 3.5, (TOKENS, D), jnp.float32)
    return (base * row_scale * column_scale).astype(jnp.bfloat16)


def shard_levels(own_key, dims, pieces, least, high):
    loudness = 1.0
    for dim, shards_of in pieces:
        draws = jax.random.uniform(jax.random.fold_in(jax.random.fold_in(own_key, 6), dim), (shards_of,), jnp.float32, least / len(pieces), high / len(pieces))
        loudness = loudness * jnp.repeat(jnp.exp(draws), dims[dim] // shards_of).reshape((-1,) + (1,) * (len(dims) - 1 - dim))
    return loudness


def deal_out(key, own, number, rows, number_of, top, reach, skew):
    sequence = jax.random.permutation(key, number_of)
    crowded, ordinary = load_shares(number_of, rows * top, reach, skew, True), load_shares(number_of, rows * top, reach, skew, False)
    places = jnp.arange(number_of)

    def named(tallies, turn):
        used = int((tallies > 0).sum())
        fixed = max(1, used // 4)
        passed = fixed + (places - fixed + turn * (used - fixed)) % max(1, number_of - fixed)
        return jnp.zeros((number_of,), jnp.int32).at[sequence[jnp.where(places < fixed, places, passed)]].set(jnp.asarray(tallies, jnp.int32))

    tallies = jnp.where(number % 4 == 0, named(crowded, number // 4), named(ordinary, number - number // 4 - 1))
    mixed = jax.random.permutation(jax.random.fold_in(own, 3), number_of)
    source_of, sink = mixed[0:number_of // 2 * 2:2], mixed[1:number_of // 2 * 2:2]
    slack = jnp.minimum(tallies[source_of] - 1, reach - tallies[sink]) // 2
    slack = jnp.where((source_of == sequence[0]) | (sink == sequence[0]) | (tallies[sink] == 0), 0, jnp.maximum(slack, 0))
    passed = jax.random.randint(jax.random.fold_in(own, 4), (number_of // 2,), 0, 1 << 20) % (slack + 1)
    tallies = tallies.at[source_of].add(-passed).at[sink].add(passed)
    items = jnp.searchsorted(jnp.cumsum(tallies), jnp.arange(rows * top), side="right").astype(jnp.int32)
    grid = items.reshape(top, rows).T
    grid = grid[jax.random.permutation(jax.random.fold_in(own, 1), rows)]
    turn = jax.random.randint(jax.random.fold_in(own, 2), (rows, 1), 0, top)
    return jnp.take_along_axis(grid, (jnp.arange(top)[None, :] + turn) % top, axis=1)


def load_shares(count, total, reach, slope, full):
    weights = [(1 << 20) // math.isqrt(standing ** slope) + 1 for standing in range(1, count + 1)]
    largest = reach if full else min(reach, max(-(-total // count), total * weights[0] // sum(weights)))
    least = 1 if total - largest >= count - 1 else 0
    given, rest = [largest] + [least] * (count - 1), total - largest - least * (count - 1)
    while rest > 0:
        free = [i for i in range(1, count) if given[i] < largest] or [i for i in range(1, count) if given[i] < reach]
        mass, remaining = sum([weights[i] for i in free]), rest
        for i in free:
            addition = min(reach - given[i], max(1, remaining * weights[i] // mass), rest)
            given[i] = given[i] + addition
            rest = rest - addition
    return np.array(given)


def scatter_about(rng, shape, scale, limit, shards=(), held_as=jnp.bfloat16):
    level = shard_levels(rng, shape, shards, -0.22, 0.18) if shards else 1.0
    values = jax.random.normal(rng, shape, jnp.float32) * scale * level
    return jnp.minimum(jnp.maximum(values, -limit), limit).astype(held_as)


def setup_inputs(seed: int = 0) -> dict:
    streams_of = jax.random.split(jax.random.key(seed), 8)
    residual = draw_residual(jax.random.fold_in(streams_of[7], 71), 0)
    norm_gain = jnp.clip(1.0 + 0.15 * jax.random.normal(streams_of[1], (D,), jnp.float32), 0.25, 1.75)
    router_weight = scatter_about(streams_of[2], (D, EXPERTS), D ** -0.5, 0.109375)
    out_grad = scatter_about(streams_of[3], (TOKENS, D), 1.0, 6.0, ((0, 128),))
    expert_ids_keys = jax.random.split(jax.random.fold_in(streams_of[4], 1), TOKENS // TOK_DEV)
    expert_ids_turns = jax.random.permutation(jax.random.fold_in(streams_of[4], 3), TOKENS // TOK_DEV)
    expert_ids = jax.vmap(lambda own, number: deal_out(jax.random.fold_in(streams_of[4], 2), own, number, TOK_DEV, EXPERTS, TOPK, CAP, 2))(expert_ids_keys, expert_ids_turns).reshape((TOKENS, TOPK))
    hidden = scatter_about(streams_of[5], (EXPERTS, SLOTS, FF), 0.05, 0.3125, ((0, 128),))
    down_weight = scatter_about(streams_of[6], (EXPERTS, FF, D), FF ** -0.5, 0.15625, ((0, 128),))
    return {"residual": residual, "norm_gain": norm_gain, "router_weight": router_weight, "out_grad": out_grad, "expert_ids": expert_ids, "hidden": hidden, "down_weight": down_weight}


def expert_step(packed):
    sent_grad, sent_prob, hidden_rows, weight = packed
    inner = lax.dot_general(sent_grad, weight, (((1,), (1,)), ((), ())), preferred_element_type=jnp.float32)
    slot_score = lax.optimization_barrier(jnp.sum(inner * hidden_rows.astype(jnp.float32), -1))
    weight_col = sent_prob.astype(jnp.float32)[:, None]
    hidden_grad = (weight_col * inner).astype(jnp.bfloat16)
    scaled = (weight_col * sent_grad.astype(jnp.float32)).astype(jnp.bfloat16)
    weight_grad = lax.dot_general(hidden_rows, scaled, (((0,), (0,)), ((), ())), preferred_element_type=jnp.float32)
    return (slot_score, hidden_grad, weight_grad.astype(jnp.bfloat16))

def reference(residual, norm_gain, router_weight, out_grad, expert_ids, hidden, down_weight):
    sources = N_EP * N_DP
    floated = residual.astype(jnp.float32)
    inverse = lax.rsqrt(lax.optimization_barrier(jnp.mean(floated * floated, -1, keepdims=True)) + 1e-05)
    unit = floated * inverse
    normed = (unit * norm_gain).astype(jnp.bfloat16)
    logits = jnp.dot(normed, router_weight, preferred_element_type=jnp.float32)
    picked = jnp.take_along_axis(logits, expert_ids, 1)
    expo = jnp.exp(picked)
    prob = expo / lax.optimization_barrier(jnp.sum(expo, -1, keepdims=True))
    flat_ids = expert_ids.reshape(sources, TOK_DEV * TOPK)
    onehot = (flat_ids[:, :, None] == jnp.arange(EXPERTS, dtype=jnp.int32)[None, None, :]).astype(jnp.int32)
    before = jnp.cumsum(onehot, 1) - onehot
    slot_rank = lax.optimization_barrier(jnp.sum(before * onehot, -1))
    source_idx = jnp.arange(sources, dtype=jnp.int32)[:, None]
    place = (flat_ids * SLOTS + source_idx * CAP + slot_rank).reshape(-1).astype(jnp.int32)
    repeated = jnp.repeat(out_grad, TOPK, axis=0)
    sent_grad = jnp.zeros((EXPERTS * SLOTS, D), jnp.bfloat16).at[place].set(repeated).reshape(EXPERTS, SLOTS, D)
    sent_prob = jnp.zeros((EXPERTS * SLOTS,), jnp.bfloat16).at[place].set(prob.astype(jnp.bfloat16).reshape(-1)).reshape(EXPERTS, SLOTS)
    slot_score, hidden_grad, down_weight_grad = lax.map(expert_step, (sent_grad, sent_prob, hidden, down_weight))
    score = slot_score.reshape(-1)[place].reshape(TOKENS, TOPK)
    pick_grad = prob * (score - lax.optimization_barrier(jnp.sum(prob * score, -1, keepdims=True)))
    match = expert_ids[:, :, None] == jnp.arange(EXPERTS, dtype=jnp.int32)[None, None, :]
    logit_grad = lax.optimization_barrier(jnp.sum(jnp.where(match, pick_grad[:, :, None], jnp.float32(0.0)), 1))
    router_grad = jnp.dot(normed.astype(jnp.float32).T, logit_grad, precision=lax.Precision.HIGHEST)
    normed_grad = jnp.dot(logit_grad, router_weight.astype(jnp.float32).T, precision=lax.Precision.HIGHEST)
    gain_grad = lax.optimization_barrier(jnp.sum(normed_grad * unit, 0))
    upper = normed_grad * norm_gain
    residual_grad = (inverse * (upper - unit * lax.optimization_barrier(jnp.mean(upper * unit, -1, keepdims=True)))).astype(jnp.bfloat16)
    return (hidden_grad, down_weight_grad, residual_grad, router_grad, gain_grad)
```

```python
import functools

import jax
import jax.numpy as jnp
from jax import lax
from jax.experimental import pallas as pl
from jax.experimental.pallas import tpu as pltpu
from jax.sharding import Mesh
from jax.sharding import PartitionSpec as P

AX = ("ep_0", "ep_1", "ep_2", "dp")
SZ = (4, 4, 2, 4)
Z, X, CORE, Y = 0, 1, 2, 3
STRIDE = (32, 8, 4, 1)
MESH = pl.DeviceIdType.MESH
D = 2880
FF = 1440
BF = jnp.bfloat16
F32 = jnp.float32

PLAN = (
    (2560, 320, 384, Y, Z, X),
    (0, 512, 512, Y, X, Z),
    (512, 512, 512, Y, Z, X),
    (1024, 512, 512, Y, X, Z),
    (1536, 512, 512, Y, Z, X),
    (2048, 512, 512, Y, X, Z),
)
NCH = len(PLAN)
GDIMS = tuple(dict.fromkeys(c[3] for c in PLAN))
FBLK = ((0, 512), (512, 512), (1024, 416))
COLORS = ((Z, (X, CORE, Y)), (X, (Z, CORE, Y)), (Y, (Z, X, CORE)))
OTHER = {Z: (X, CORE, Y), X: (Z, CORE, Y), Y: (Z, X, CORE)}


def off(**kw):
    return kw


def plane_offsets(dims):
    out = []
    for a in range(SZ[dims[0]]):
        for b in range(SZ[dims[1]]):
            for c in range(SZ[dims[2]]):
                if (a, b, c) != (0, 0, 0):
                    t = [0, 0, 0, 0]
                    t[dims[0]], t[dims[1]], t[dims[2]] = a, b, c
                    out.append(tuple(t))
    return out


def spread(offsets):
    def hops(t):
        return sum(min(t[i], SZ[i] - t[i]) for i in (Z, X, Y))

    return sorted(offsets, key=lambda t: -hops(t))


def ring_offset(dim, d):
    t = [0, 0, 0, 0]
    t[dim] = d
    return tuple(t)


def all_peers():
    peers = []
    for c in PLAN:
        for d in (1, 2, 3):
            peers += [ring_offset(c[3], d), ring_offset(c[4], d)]
        for dq in range(4):
            for dc in range(2):
                if dq or dc:
                    t = [0, 0, 0, 0]
                    t[c[5]], t[CORE] = dq, dc
                    peers.append(tuple(t))
    peers += plane_offsets((Z, X, CORE))
    peers += [ring_offset(Y, d) for d in (1, 2, 3)]
    for a, others in COLORS:
        peers += [ring_offset(a, d) for d in (1, 2, 3)]
        peers += plane_offsets(others)
    return list(dict.fromkeys(peers))


PEERS = all_peers()


def inverse_of(t):
    return tuple((SZ[i] - t[i]) % SZ[i] for i in range(4))


def kernel(*refs):
    names = (
        ["og", "res", "gain", "rw", "ids", "hid_h", "w_h"]
        + ["hg_h", "sc_h", "rg", "tot"]
        + ["hid", "w", "acc", "hgs", "mt", "prob", "probb", "normed", "normedt", "unit"]
        + ["rsc", "rr", "xs", "ar1", "as2", "ar2", "gv", "rag"]
    )
    names += [f"mg{g}" for g in range(len(GDIMS))] + ["pg"] + [f"pb{g}" for g in range(len(GDIMS))]
    for i in range(NCH):
        names += [f"tok{i}", f"sb{i}", f"b1_{i}", f"fin{i}", f"scs{i}"]
    names += ["s_m", "r_m", "s_p", "r_p", "s_ag", "r_ag", "s_p1", "r_p1", "s_p2", "r_p2"]
    names += ["s_ret", "r_ret", "s_rety", "r_rety", "s_a1", "r_a1", "s_a2", "r_a2"]
    names += ["s_g2", "r_g2", "s_g1", "r_g1", "loc"]
    assert len(names) == len(refs)
    k = dict(zip(names, refs))
    me = [lax.axis_index(a) for a in AX]

    def dev(t):
        return tuple(
            lax.rem(me[i] + t[i], SZ[i]) if t[i] else me[i] for i in range(4)
        )

    def coord(dim, d):
        return lax.rem(me[dim] + d, SZ[dim]) if d else me[dim]

    def remote(src, dst, ssem, rsem, t):
        return pltpu.make_async_remote_copy(
            src_ref=src, dst_ref=dst, send_sem=ssem, recv_sem=rsem,
            device_id=dev(t), device_id_type=MESH,
        )

    pending = []

    def launch(src, dst, ssem, rsem, t):
        cp = remote(src, dst, ssem, rsem, t)
        cp.start()
        pending.append(cp)
        return cp

    barrier = pltpu.get_barrier_semaphore()
    for t in PEERS:
        pl.semaphore_signal(barrier, inc=1, device_id=dev(t), device_id_type=MESH)
    w_copy = pltpu.make_async_copy(k["w_h"], k["w"], k["loc"].at[0])
    w_copy.start()
    hid_copy = pltpu.make_async_copy(k["hid_h"], k["hid"], k["loc"].at[1])
    hid_copy.start()

    e_row = lax.broadcasted_iota(jnp.int32, (128, 128), 0)
    t_col = lax.broadcasted_iota(jnp.int32, (128, 128), 1)
    match = e_row == k["ids"][0:1, :]
    for j in range(1, 4):
        match = match | (e_row == k["ids"][j : j + 1, :])
    matchf = match.astype(F32)
    earlier = jnp.where(e_row < t_col, 1.0, 0.0).astype(BF)
    count = jnp.dot(matchf.astype(BF), earlier, preferred_element_type=F32)
    mt = matchf * (count + 1.0)
    k["mt"][...] = mt
    for g, a in enumerate(GDIMS):
        k[f"mg{g}"][me[a]] = mt.astype(BF)
    k["rag"][...] = jnp.zeros_like(k["rag"])
    k["rag"][:, 0:320] = k["og"][:, 2560:2880]
    pl.semaphore_wait(barrier, len(PEERS))

    m_cp = []
    for g, a in enumerate(GDIMS):
        own = k[f"mg{g}"].at[me[a]]
        m_cp.append([
            launch(own, own, k["s_m"].at[g, d - 1], k["r_m"].at[g, d - 1], ring_offset(a, d))
            for d in (2, 1, 3)
        ])
    ag = []
    for i, (c0, nc, cw, a, p, q) in enumerate(PLAN):
        src = k["rag"] if nc != cw else k["og"].at[:, pl.ds(c0, nc)]
        ag.append([
            launch(src, k[f"tok{i}"].at[me[a]], k["s_ag"].at[i, d - 1], k["r_ag"].at[i, d - 1], ring_offset(a, d))
            for d in (2, 1, 3)
        ])

    floated = k["res"][...].astype(F32)
    inv = lax.rsqrt(jnp.mean(floated * floated, -1, keepdims=True) + 1e-05)
    unit = floated * inv
    normed = (unit * k["gain"][...]).astype(BF)
    logits = jnp.dot(normed, k["rw"][...], preferred_element_type=F32)
    k["normed"][...] = normed
    expo = jnp.where(match, jnp.exp(logits.T), 0.0)
    prob = expo / jnp.sum(expo, 0, keepdims=True)
    k["prob"][...] = prob
    pa = PLAN[0][3]
    k["pg"][me[pa]] = prob.astype(BF)
    own = k["pg"].at[me[pa]]
    p_cp = [
        launch(own, own, k["s_p"].at[d - 1], k["r_p"].at[d - 1], ring_offset(pa, d)) for d in (2, 1, 3)
    ]
    for i, (c0, nc, cw, a, p, q) in enumerate(PLAN):
        k[f"tok{i}"][me[a]] = k["rag"][...] if nc != cw else k["og"][:, c0 : c0 + nc]

    group = lax.broadcasted_iota(jnp.int32, (32, 24, 128), 0)
    inner_row = lax.broadcasted_iota(jnp.int32, (32, 24, 128), 1)
    lane3 = lax.broadcasted_iota(jnp.int32, (32, 24, 128), 2)
    src_of = (
        jnp.where(inner_row >= 6, 1, 0) + jnp.where(inner_row >= 12, 1, 0) + jnp.where(inner_row >= 18, 1, 0)
    )
    want = (inner_row - 6 * src_of + 1).astype(F32).reshape(768, 128)
    src_flat = src_of.reshape(768, 128)

    def pick_matrix(a, p, q):
        dp, qq, cc = group // 8, (group // 2) % 4, group % 2
        pp = (me[p] + dp) % 4
        expert = STRIDE[a] * me[a] + STRIDE[p] * pp + STRIDE[q] * qq + STRIDE[CORE] * cc
        return jnp.where(expert == lane3, 1.0, 0.0).reshape(768, 128).astype(BF)

    sent = None
    built = None
    p1 = []
    for i, (c0, nc, cw, a, p, q) in enumerate(PLAN):
        g = GDIMS.index(a)
        pb = k[f"pb{g}"]
        if i < len(GDIMS):
            for cp in m_cp[g]:
                cp.wait_recv()
        if i < len(GDIMS) or built[g] != (p, q):
            pick = pick_matrix(a, p, q)
            if i == 0:
                for cp in p_cp:
                    cp.wait_recv()
                sent = jnp.zeros((768, 1), F32)
            for s in range(4):
                marks = jnp.dot(pick, k[f"mg{g}"][s], preferred_element_type=F32)
                hit = (marks == want) & (src_flat == s)
                pb[:, s * 128 : (s + 1) * 128] = jnp.where(hit, 1.0, 0.0).astype(BF)
                if i == 0:
                    weights = jnp.dot(pick, k["pg"][s], preferred_element_type=F32)
                    sent = sent + jnp.sum(jnp.where(hit, weights, 0.0), -1, keepdims=True)
            built = dict(built or {})
            built[g] = (p, q)
        for cp in ag[i]:
            cp.wait_recv()
        rows = jnp.dot(pb[...], k[f"tok{i}"][...].reshape(512, cw), preferred_element_type=F32)
        if i == 0:
            lane = lax.broadcasted_iota(jnp.int32, (768, cw), 1)
            rows = jnp.where(lane >= nc, sent, rows)
        rows = rows.reshape(4, 8, 3, 8, cw).astype(BF)
        k[f"sb{i}"][...] = rows[1:]
        k[f"b1_{i}"][me[p]] = rows[0]
        p1.append([
            launch(k[f"sb{i}"].at[d - 1], k[f"b1_{i}"].at[me[p]], k["s_p1"].at[i, d - 1], k["r_p1"].at[i, d - 1], ring_offset(p, d))
            for d in (2, 1, 3)
        ])

    p2 = []
    for i, (c0, nc, cw, a, p, q) in enumerate(PLAN):
        for cp in p1[i]:
            cp.wait_recv()
        others = OTHER[a]
        spot = tuple(slice(None) if o == p else me[o] for o in others)
        b1, fin = k[f"b1_{i}"], k[f"fin{i}"]
        cps = []
        n = 0
        for dq in (2, 1, 3, 0):
            for dc in (0, 1):
                if dq == 0 and dc == 0:
                    continue
                t = [0, 0, 0, 0]
                t[q], t[CORE] = dq, dc
                slot = coord(q, dq) * 2 + coord(CORE, dc)
                cps.append(launch(b1.at[:, slot], fin.at[spot], k["s_p2"].at[i, n], k["r_p2"].at[i, n], tuple(t)))
                n += 1
        p2.append(cps)
        fin[spot] = b1[:, me[q] * 2 + me[CORE]]

    k["normedt"][...] = normed.astype(F32).T.astype(BF)
    w_copy.wait()
    hid_copy.wait()

    weight_col = None
    out_cps = []
    for i, (c0, nc, cw, a, p, q) in enumerate(PLAN):
        for cp in p2[i]:
            cp.wait_recv()
        rows = k[f"fin{i}"][...].reshape(96, 8, cw).astype(F32).reshape(768, cw)
        if i == 0:
            weight_col = rows[:, nc : nc + 1]
            rows = rows[:, :nc]
        rows_b = rows.astype(BF)
        k[f"scs{i}"][...] = (weight_col * rows).astype(BF)
        cp = pltpu.make_async_copy(k[f"scs{i}"], k["sc_h"].at[:, pl.ds(c0, nc)], k["loc"].at[2 + i])
        cp.start()
        out_cps.append(cp)
        for f0, fn in FBLK:
            part = lax.dot_general(
                rows_b, k["w"][f0 : f0 + fn, c0 : c0 + nc], (((1,), (1,)), ((), ())), preferred_element_type=F32
            )
            if i == 0:
                k["acc"][:, f0 : f0 + fn] = part
            else:
                k["acc"][:, f0 : f0 + fn] += part

    slot_score = jnp.zeros((768, 1), F32)
    for f0, fn in FBLK:
        slot_score = slot_score + jnp.sum(
            k["acc"][:, f0 : f0 + fn] * k["hid"][:, f0 : f0 + fn].astype(F32), -1, keepdims=True
        )
    packed = jnp.sum(jnp.where(lane3 == inner_row, slot_score.reshape(32, 24, 1), 0.0), 1)
    k["rsc"][...] = packed.reshape(32, 1, 128)
    mine = me[Z] * 8 + me[X] * 2 + me[CORE]
    for t in spread(plane_offsets((Z, X, CORE))):
        there = coord(Z, t[Z]) * 8 + coord(X, t[X]) * 2 + coord(CORE, t[CORE])
        cp = remote(k["rsc"].at[there], k["rr"].at[mine, me[Y]], k["s_ret"], k["r_ret"], t)
        cp.start()
    k["rr"][mine, me[Y]] = k["rsc"][mine]
    for f0, fn in FBLK:
        k["hgs"][:, f0 : f0 + fn] = (weight_col * k["acc"][:, f0 : f0 + fn]).astype(BF)
    cp = pltpu.make_async_copy(k["hgs"], k["hg_h"], k["loc"].at[2 + NCH])
    cp.start()
    out_cps.append(cp)
    few = k["rsc"].at[pl.ds(0, 31)]
    pltpu.make_async_copy(few, few, k["r_ret"]).wait()
    column = k["rr"].at[:, me[Y]]
    y_cp = [
        launch(column, column, k["s_rety"].at[d - 1], k["r_rety"].at[d - 1], ring_offset(Y, d)) for d in (2, 1, 3)
    ]
    for cp in y_cp:
        cp.wait_recv()

    back = k["rr"][...].reshape(128, 128)
    mt = k["mt"][...]
    prob = k["prob"][...]
    score = jnp.zeros((128, 128), F32)
    for r in range(6):
        one = jnp.sum(jnp.where(t_col == 6 * me[Y] + r, back, 0.0), -1, keepdims=True)
        score = score + jnp.where(mt == float(r + 1), one, 0.0)
    grad_t = prob * (score - jnp.sum(prob * score, 0, keepdims=True))
    grad = grad_t.T
    hi = grad.astype(BF)
    lo = (grad - hi.astype(F32)).astype(BF)
    local = jnp.dot(k["normedt"][...], hi, preferred_element_type=F32) + jnp.dot(
        k["normedt"][...], lo, preferred_element_type=F32
    )
    nt = (((1,), (1,)), ((), ()))
    normed_grad = lax.dot_general(hi, k["rw"][...], nt, preferred_element_type=F32) + lax.dot_general(
        lo, k["rw"][...], nt, preferred_element_type=F32
    )
    floated = k["res"][...].astype(F32)
    inv = lax.rsqrt(jnp.mean(floated * floated, -1, keepdims=True) + 1e-05)
    unit = floated * inv
    gain_local = jnp.sum(normed_grad * unit, 0, keepdims=True)
    k["gv"][...] = jnp.zeros_like(k["gv"])
    for j in range(22):
        k["gv"][j : j + 1, :] = gain_local[:, j * 128 : (j + 1) * 128]
    k["gv"][22:23, 0:64] = gain_local[:, 2816:2880]
    xs = k["xs"]
    xs[pl.ds(0, 360)] = local.reshape(360, 8, 128).astype(BF)
    xs[pl.ds(360, 3)] = k["gv"][...].reshape(3, 8, 128).astype(BF)
    xs[pl.ds(363, 21)] = jnp.zeros((21, 8, 128), BF)

    a1 = []
    for n, (a, others) in enumerate(COLORS):
        for d in (2, 1, 3):
            piece = xs.at[pl.ds(pl.multiple_of(128 * n + 32 * coord(a, d), 32), 32)]
            a1.append(launch(piece, k["ar1"].at[n, d - 1], k["s_a1"].at[n, d - 1], k["r_a1"].at[n, d - 1], ring_offset(a, d)))
    upper = normed_grad * k["gain"][...]
    k["rg"][...] = (inv * (upper - unit * jnp.mean(upper * unit, -1, keepdims=True))).astype(BF)

    for n, (a, others) in enumerate(COLORS):
        for cp in a1[3 * n : 3 * n + 3]:
            cp.wait_recv()
        total = xs[pl.ds(pl.multiple_of(128 * n + 32 * me[a], 32), 32)].astype(F32)
        for d in range(3):
            total = total + k["ar1"][n, d].astype(F32)
        k["as2"][n] = total.astype(BF)
        ring = (SZ[others[1]] * SZ[others[2]], SZ[others[2]], 1)

        def rank(t):
            return sum(coord(o, t[o]) * s for o, s in zip(others, ring))

        here = rank((0, 0, 0, 0))
        for t in spread(plane_offsets(others)):
            cp = remote(k["as2"].at[n, rank(t)], k["ar2"].at[n, here], k["s_a2"].at[n], k["r_a2"].at[n], t)
            cp.start()
        k["ar2"][n, here] = k["as2"][n, here]
    tot = k["tot"]
    for n, (a, others) in enumerate(COLORS):
        few = k["as2"].at[n, pl.ds(0, 31)]
        pltpu.make_async_copy(few, few, k["r_a2"].at[n]).wait()
        ring = (SZ[others[1]] * SZ[others[2]], SZ[others[2]], 1)
        here = sum(me[o] * s for o, s in zip(others, ring))
        done = jnp.sum(k["ar2"][n].astype(F32), 0)
        at = 128 * n + 32 * me[a] + here
        tot[at] = done.astype(BF)
        for t in spread(plane_offsets(others)):
            cp = remote(tot.at[at], tot.at[at], k["s_g2"].at[n], k["r_g2"].at[n], t)
            cp.start()
    g1 = []
    for n, (a, others) in enumerate(COLORS):
        few = k["as2"].at[n, pl.ds(0, 31)]
        pltpu.make_async_copy(few, few, k["r_g2"].at[n]).wait()
        piece = tot.at[pl.ds(pl.multiple_of(128 * n + 32 * me[a], 32), 32)]
        for d in (2, 1, 3):
            g1.append(launch(piece, piece, k["s_g1"].at[n, d - 1], k["r_g1"].at[n, d - 1], ring_offset(a, d)))
    for cp in g1:
        cp.wait_recv()
    for cp in pending:
        cp.wait_send()
    few = k["rsc"].at[pl.ds(0, 31)]
    pltpu.make_async_copy(few, few, k["s_ret"]).wait()
    for n in range(3):
        few = k["as2"].at[n, pl.ds(0, 31)]
        pltpu.make_async_copy(few, few, k["s_a2"].at[n]).wait()
        pltpu.make_async_copy(few, few, k["s_g2"].at[n]).wait()
    for cp in out_cps:
        cp.wait()


def on_device(residual, norm_gain, router_weight, out_grad, expert_ids, hidden, down_weight):
    vm = pl.BlockSpec(memory_space=pltpu.VMEM)
    hbm = pl.BlockSpec(memory_space=pl.ANY)
    dma = pltpu.SemaphoreType.DMA
    scratch = [
        pltpu.VMEM((768, FF), BF), pltpu.VMEM((FF, D), BF), pltpu.VMEM((768, FF), F32), pltpu.VMEM((768, FF), BF),
        pltpu.VMEM((128, 128), F32), pltpu.VMEM((128, 128), F32), pltpu.VMEM((128, 128), BF),
        pltpu.VMEM((128, D), BF), pltpu.VMEM((D, 128), BF), pltpu.VMEM((8, 128), F32),
        pltpu.VMEM((32, 1, 128), F32), pltpu.VMEM((32, 4, 1, 128), F32),
        pltpu.VMEM((384, 8, 128), BF), pltpu.VMEM((3, 3, 32, 8, 128), BF), pltpu.VMEM((3, 32, 8, 128), BF),
        pltpu.VMEM((3, 32, 8, 128), BF), pltpu.VMEM((24, 128), F32), pltpu.VMEM((128, 384), BF),
    ]
    scratch += [pltpu.VMEM((4, 128, 128), BF) for _ in GDIMS]
    scratch += [pltpu.VMEM((4, 128, 128), BF)]
    scratch += [pltpu.VMEM((768, 512), BF) for _ in GDIMS]
    for c0, nc, cw, a, p, q in PLAN:
        sizes = tuple(SZ[o] for o in OTHER[a])
        scratch += [
            pltpu.VMEM((4, 128, cw), BF), pltpu.VMEM((3, 8, 3, 8, cw), BF), pltpu.VMEM((4, 8, 3, 8, cw), BF),
            pltpu.VMEM(sizes + (3, 8, cw), BF), pltpu.VMEM((768, nc), BF),
        ]
    ng = len(GDIMS)
    scratch += [dma((ng, 3)), dma((ng, 3)), dma((3,)), dma((3,)), dma((NCH, 3)), dma((NCH, 3))]
    scratch += [dma((NCH, 3)), dma((NCH, 3)), dma((NCH, 7)), dma((NCH, 7))]
    scratch += [dma(()), dma(()), dma((3,)), dma((3,)), dma((3, 3)), dma((3, 3)), dma((3,)), dma((3,))]
    scratch += [dma((3,)), dma((3,)), dma((3, 3)), dma((3, 3)), dma((3 + NCH,))]
    hidden_grad, scaled, residual_grad, total = pl.pallas_call(
        kernel,
        name="routed",
        out_shape=(
            jax.ShapeDtypeStruct((768, FF), BF),
            jax.ShapeDtypeStruct((768, D), BF),
            jax.ShapeDtypeStruct((128, D), BF),
            jax.ShapeDtypeStruct((384, 8, 128), BF),
        ),
        in_specs=[vm, vm, vm, vm, vm, hbm, hbm],
        out_specs=(hbm, hbm, vm, vm),
        scratch_shapes=scratch,
        compiler_params=pltpu.CompilerParams(
            collective_id=0, has_side_effects=True, vmem_limit_bytes=67043328
        ),
    )(out_grad, residual, norm_gain[None], router_weight, expert_ids.T, hidden[0], down_weight[0])
    weight_grad = lax.dot_general(
        hidden[0], scaled, (((0,), (0,)), ((), ())), preferred_element_type=F32
    )
    router_grad = total[:360].reshape(D, 128).astype(F32)
    gain_grad = total[360:363].reshape(3072)[:D].astype(F32)
    return hidden_grad[None], weight_grad.astype(BF)[None], residual_grad, router_grad, gain_grad


def solution(mesh):
    finer = Mesh(mesh.devices.reshape(4, 4, 2, mesh.shape["dp"]), AX)
    rows = P(AX, None)
    cube = P(AX, None, None)
    return jax.shard_map(
        on_device,
        mesh=finer,
        in_specs=(rows, P(), P(), rows, rows, cube, cube),
        out_specs=(cube, cube, rows, P(), P()),
        check_vma=False,
    )
```

```python
import functools

import jax
import jax.numpy as jnp
from jax import lax
from jax.experimental import pallas as pl
from jax.experimental.pallas import tpu as pltpu
from jax.sharding import Mesh
from jax.sharding import PartitionSpec as P

AX = ("ep_0", "ep_1", "ep_2", "dp")
SZ = (4, 4, 2, 4)
Z, X, CORE, Y = 0, 1, 2, 3
STRIDE = (32, 8, 4, 1)
MESH = pl.DeviceIdType.MESH
D = 2880
FF = 1440
BF = jnp.bfloat16
F32 = jnp.float32

PLAN = (
    (0, 640, 640, Y, Z, X),
    (640, 640, 640, Z, X, Y),
    (1280, 640, 640, X, Y, Z),
    (1920, 384, 384, Y, X, Z),
    (2304, 384, 384, Z, Y, X),
    (2688, 192, 256, X, Z, Y),
)
NCH = len(PLAN)
LAST = NCH - 1
HALF = (0, 1920, 2880)
REUSE = {3: 0, 4: 1}
GDIMS = tuple(dict.fromkeys(c[3] for c in PLAN))
FB = 480
NT = (((1,), (1,)), ((), ()))
TN = (((0,), (0,)), ((), ()))
COLORS = ((Z, (X, CORE, Y)), (X, (Z, CORE, Y)), (Y, (Z, X, CORE)))
OTHER = {Z: (X, CORE, Y), X: (Z, CORE, Y), Y: (Z, X, CORE)}


def off(**kw):
    return kw


def plane_offsets(dims):
    out = []
    for a in range(SZ[dims[0]]):
        for b in range(SZ[dims[1]]):
            for c in range(SZ[dims[2]]):
                if (a, b, c) != (0, 0, 0):
                    t = [0, 0, 0, 0]
                    t[dims[0]], t[dims[1]], t[dims[2]] = a, b, c
                    out.append(tuple(t))
    return out


def spread(offsets):
    def hops(t):
        return sum(min(t[i], SZ[i] - t[i]) for i in (Z, X, Y))

    return sorted(offsets, key=lambda t: -hops(t))


def ring_offset(dim, d):
    t = [0, 0, 0, 0]
    t[dim] = d
    return tuple(t)


def all_peers():
    peers = []
    for c in PLAN:
        for d in (1, 2, 3):
            peers += [ring_offset(c[3], d), ring_offset(c[4], d)]
        for dq in range(4):
            for dc in range(2):
                if dq or dc:
                    t = [0, 0, 0, 0]
                    t[c[5]], t[CORE] = dq, dc
                    peers.append(tuple(t))
    peers += plane_offsets((Z, X, CORE))
    peers += [ring_offset(Y, d) for d in (1, 2, 3)]
    for a, others in COLORS:
        peers += [ring_offset(a, d) for d in (1, 2, 3)]
        peers += plane_offsets(others)
    return list(dict.fromkeys(peers))


PEERS = all_peers()


def inverse_of(t):
    return tuple((SZ[i] - t[i]) % SZ[i] for i in range(4))


def kernel(*refs):
    names = (
        ["og", "res", "gain", "rw", "ids", "hid_h", "w_h"]
        + ["hg_h", "wg_h", "rg", "tot"]
        + ["hid", "w", "acc", "hgs", "mt", "prob", "normedt", "gc"]
        + ["rsc", "rr", "xs", "ar1", "as2", "ar2", "gv", "rows"]
    )
    ng = len(GDIMS)
    names += [f"mg{g}" for g in range(ng)] + ["pg"] + [f"pb{g}" for g in range(ng)]
    names += [f"pick{g}" for g in range(ng)]
    names += [f"perm{a}" for a in (Z, X)]
    for i in range(NCH):
        names += [f"tok{i}", f"sel{i}", f"b1_{i}", f"fin{i}"] + ([f"wgs{i}"] if i not in REUSE else [])
    names += ["s_m", "r_m", "s_p", "r_p", "s_ag", "r_ag", "s_p1", "r_p1", "s_p2", "r_p2"]
    names += ["s_ret", "r_ret", "s_rety", "r_rety", "s_a1", "r_a1", "s_a2", "r_a2"]
    names += ["s_g2", "r_g2", "s_g1", "r_g1", "loc"]
    assert len(names) == len(refs)
    k = dict(zip(names, refs))
    me = [lax.axis_index(a) for a in AX]

    def dev(t):
        return tuple(
            lax.rem(me[i] + t[i], SZ[i]) if t[i] else me[i] for i in range(4)
        )

    def coord(dim, d):
        return lax.rem(me[dim] + d, SZ[dim]) if d else me[dim]

    def remote(src, dst, ssem, rsem, t):
        return pltpu.make_async_remote_copy(
            src_ref=src, dst_ref=dst, send_sem=ssem, recv_sem=rsem,
            device_id=dev(t), device_id_type=MESH,
        )

    pending = []

    def launch(src, dst, ssem, rsem, t):
        cp = remote(src, dst, ssem, rsem, t)
        cp.start()
        pending.append(cp)
        return cp

    barrier = pltpu.get_barrier_semaphore()
    for t in PEERS:
        pl.semaphore_signal(barrier, inc=1, device_id=dev(t), device_id_type=MESH)
    w_copy = pltpu.make_async_copy(k["w_h"], k["w"], k["loc"].at[0])
    w_copy.start()
    hid_copy = pltpu.make_async_copy(k["hid_h"], k["hid"], k["loc"].at[1])
    hid_copy.start()

    e_row = lax.broadcasted_iota(jnp.int32, (128, 128), 0)
    t_col = lax.broadcasted_iota(jnp.int32, (128, 128), 1)
    match = e_row == k["ids"][0:1, :]
    for j in range(1, 4):
        match = match | (e_row == k["ids"][j : j + 1, :])
    matchf = match.astype(F32)
    earlier = jnp.where(e_row < t_col, 1.0, 0.0).astype(BF)
    count = jnp.dot(matchf.astype(BF), earlier, preferred_element_type=F32)
    mt = matchf * (count + 1.0)
    k["mt"][...] = mt
    for g, a in enumerate(GDIMS):
        k[f"mg{g}"][me[a]] = mt.astype(BF)
    nl, cl = PLAN[LAST][1:3]
    k[f"tok{LAST}"][nl:cl, :] = jnp.zeros((cl - nl, 512), BF)

    group = lax.broadcasted_iota(jnp.int32, (32, 24, 128), 0)
    inner_row = lax.broadcasted_iota(jnp.int32, (32, 24, 128), 1)
    lane3 = lax.broadcasted_iota(jnp.int32, (32, 24, 128), 2)
    src_of = (
        jnp.where(inner_row >= 6, 1, 0) + jnp.where(inner_row >= 12, 1, 0) + jnp.where(inner_row >= 18, 1, 0)
    )
    want = (inner_row - 6 * src_of + 1).astype(F32).reshape(768, 128)
    src_flat = src_of.reshape(768, 128)
    for g, a in enumerate(GDIMS):
        o = OTHER[a]
        n1, n2 = SZ[o[1]] * SZ[o[2]], SZ[o[2]]
        expert = STRIDE[a] * me[a] + STRIDE[o[0]] * (group // n1)
        expert = expert + STRIDE[o[1]] * ((group // n2) % SZ[o[1]]) + STRIDE[o[2]] * (group % n2)
        k[f"pick{g}"][...] = jnp.where(expert == lane3, 1.0, 0.0).reshape(768, 128).astype(BF)
    eye = e_row == t_col
    for j in range(23):
        n = min(128, D - 128 * j)
        row = k["gain"][pl.ds(128 * j, n)].reshape(1, n)
        col = jnp.sum(jnp.where(eye[:n, :n], row, 0.0), -1, keepdims=True)
        k["gc"][128 * j : 128 * j + n, :] = jnp.broadcast_to(col, (n, 128))
    pl.semaphore_wait(barrier, len(PEERS))

    m_cp = []
    for g, a in enumerate(GDIMS):
        own = k[f"mg{g}"].at[me[a]]
        m_cp.append([
            launch(own, own, k["s_m"].at[g, d - 1], k["r_m"].at[g, d - 1], ring_offset(a, d))
            for d in (2, 1, 3)
        ])
    ag = [[] for _ in PLAN]

    def gather(i, ds):
        c0, nc, cw, a, p, q = PLAN[i]
        src = k["og"].at[pl.ds(c0, nc)]
        dst = k[f"tok{i}"].at[pl.ds(0, nc), pl.ds(pl.multiple_of(me[a] * 128, 128), 128)]
        for d in ds:
            ag[i].append(
                launch(src, dst, k["s_ag"].at[i, d - 1], k["r_ag"].at[i, d - 1], ring_offset(a, d))
            )

    for i in (0, 1, 2):
        gather(i, (2, 1, 3))
    for i in (3, 4, 5):
        gather(i, (1, 3))
    for i, (c0, nc, cw, a, p, q) in enumerate(PLAN):
        k[f"tok{i}"][0:nc, pl.ds(pl.multiple_of(me[a] * 128, 128), 128)] = k["og"][c0 : c0 + nc, :]

    floated = k["res"][...].astype(F32)
    inv = lax.rsqrt(jnp.mean(floated * floated, 0, keepdims=True) + 1e-05)
    normed = (floated * inv * k["gc"][...]).astype(BF)
    k["normedt"][...] = normed
    logits = lax.dot_general(k["rw"][...], normed, TN, preferred_element_type=F32)
    expo = jnp.where(match, jnp.exp(logits), 0.0)
    prob = expo / jnp.sum(expo, 0, keepdims=True)
    k["prob"][...] = prob
    pa = PLAN[LAST][3]
    k["pg"][me[pa]] = prob.astype(BF)
    own = k["pg"].at[me[pa]]
    p_cp = [
        launch(own, own, k["s_p"].at[d - 1], k["r_p"].at[d - 1], ring_offset(pa, d)) for d in (2, 1, 3)
    ]

    p1 = {}

    def first_ring(i):
        c0, nc, cw, a, p, q = PLAN[i]
        g = GDIMS.index(a)
        pb = k[f"pb{g}"]
        if i < len(GDIMS):
            for cp in m_cp[g]:
                cp.wait_recv()
            for s in range(4):
                marks = jnp.dot(k[f"pick{g}"][...], k[f"mg{g}"][s], preferred_element_type=F32)
                hit = (marks == want) & (src_flat == s)
                pb[:, s * 128 : (s + 1) * 128] = jnp.where(hit, 1.0, 0.0).astype(BF)
        for cp in ag[i]:
            cp.wait_recv()
        rows = lax.dot_general(pb[...], k[f"tok{i}"][...], NT, preferred_element_type=F32)
        if i == LAST:
            for cp in p_cp:
                cp.wait_recv()
            sent = jnp.zeros((768, 128), F32)
            for s in range(4):
                weights = jnp.dot(k[f"pick{g}"][...], k["pg"][s], preferred_element_type=F32)
                sent = sent + pb[:, s * 128 : (s + 1) * 128].astype(F32) * weights
            sent = jnp.sum(sent, -1, keepdims=True)
            lane = lax.broadcasted_iota(jnp.int32, (768, cw), 1)
            rows = jnp.where(lane >= nc, sent, rows)
        others = OTHER[a]
        sel, b1 = k[f"sel{i}"], k[f"b1_{i}"]
        sel[...] = rows.reshape(tuple(SZ[o] for o in others) + (3, 8, cw)).astype(BF)
        cps = []
        for d in (2, 1, 3):
            spot = tuple(coord(p, d) if o == p else slice(None) for o in others)
            cps.append(launch(sel.at[spot], b1.at[me[p]], k["s_p1"].at[i, d - 1], k["r_p1"].at[i, d - 1], ring_offset(p, d)))
        p1[i] = cps
        b1[me[p]] = sel[tuple(me[p] if o == p else slice(None) for o in others)]

    for i in (0, 1, 2):
        first_ring(i)
    for i in (3, 4, 5):
        gather(i, (2,))

    slot = lax.broadcasted_iota(jnp.int32, (768, 128), 0)
    lane = lax.broadcasted_iota(jnp.int32, (768, 128), 1)
    src = (slot * 10923) // 65536
    rest = slot - 6 * src
    from_z = (src % 32) * 24 + (src // 32) * 6 + rest
    from_x = ((src // 32) * 8 + src % 8) * 24 + ((src // 8) % 4) * 6 + rest
    for a, origin in ((Z, from_z), (X, from_x)):
        for j in range(6):
            k[f"perm{a}"][:, 128 * j : 128 * j + 128] = jnp.where(origin == lane + 128 * j, 1.0, 0.0).astype(BF)
    w_copy.wait()
    hid_copy.wait()

    p2 = {}

    def second_ring(i):
        c0, nc, cw, a, p, q = PLAN[i]
        for cp in p1[i]:
            cp.wait_recv()
        others = OTHER[a]
        left = tuple(o for o in others if o != p)
        spot = tuple(slice(None) if o == p else me[o] for o in others)
        b1, fin = k[f"b1_{i}"], k[f"fin{i}"]

        def part_of(dq, dc):
            return (slice(None),) + tuple(coord(q, dq) if o == q else coord(CORE, dc) for o in left)

        cps = []
        n = 0
        for dq in (2, 1, 3, 0):
            for dc in (0, 1):
                if dq == 0 and dc == 0:
                    continue
                t = [0, 0, 0, 0]
                t[q], t[CORE] = dq, dc
                cps.append(launch(b1.at[part_of(dq, dc)], fin.at[spot], k["s_p2"].at[i, n], k["r_p2"].at[i, n], tuple(t)))
                n += 1
        p2[i] = cps
        fin[spot] = b1[part_of(0, 0)]

    def arrived(i):
        c0, nc, cw, a, p, q = PLAN[i]
        for cp in p2[i]:
            cp.wait_recv()
        rows = k[f"fin{i}"][...].reshape(96, 8, cw).astype(F32).reshape(768, cw)
        if a != Y:
            rows = jnp.dot(k[f"perm{a}"][...], rows.astype(BF), preferred_element_type=F32)
        weight = None
        if i == LAST:
            spot = lax.broadcasted_iota(jnp.int32, (16, cw), 1)
            weight = rows[:, nc : nc + 1], lax.dot_general(
                jnp.where(spot == nc, 1.0, 0.0).astype(BF), rows.astype(BF), NT, preferred_element_type=F32
            )[0:1]
            rows = rows[:, :nc]
        k["rows"][:, c0 : c0 + nc] = rows.astype(BF)
        return weight

    def inner_part(h):
        cols = slice(HALF[h], HALF[h + 1])

        def step(n, carry):
            at = pl.ds(pl.multiple_of(n * FB, FB), FB)
            part = lax.dot_general(k["w"][at, cols], k["rows"][:, cols], NT, preferred_element_type=F32)
            if h == 0:
                k["acc"][at, :] = part
            else:
                k["acc"][at, :] += part
            return carry

        lax.fori_loop(0, FF // FB, step, 0)

    for i in (0, 1, 2):
        second_ring(i)
    for i in (3, 4, 5):
        first_ring(i)
    for i in (0, 1, 2):
        arrived(i)
    for i in (3, 4, 5):
        second_ring(i)
    inner_part(0)
    for i in (3, 4, 5):
        weight = arrived(i)
    weight_col, weight_row = weight
    inner_part(1)

    out_cps = {}

    def weight_grad(i):
        c0, nc = PLAN[i][:2]
        scaled = (weight_col * k["rows"][:, c0 : c0 + nc].astype(F32)).astype(BF)
        out = k[f"wgs{REUSE.get(i, i)}"]
        if i in REUSE:
            out_cps[REUSE[i]].wait()

        def step(n, carry):
            at = pl.ds(pl.multiple_of(n * FB, FB), FB)
            out[at, 0:nc] = jnp.dot(k["hid"][at, :], scaled, preferred_element_type=F32).astype(BF)
            return carry

        lax.fori_loop(0, FF // FB, step, 0)
        src = out.at[:, pl.ds(0, nc)] if i in REUSE else out
        cp = pltpu.make_async_copy(src, k["wg_h"].at[:, pl.ds(c0, nc)], k["loc"].at[2 + i])
        cp.start()
        out_cps[i] = cp

    slot_score = jnp.sum(k["acc"][...] * k["hid"][...].astype(F32), 0, keepdims=True)
    hi = slot_score.astype(BF)
    left = slot_score - hi.astype(F32)
    mid = left.astype(BF)
    lo = (left - mid.astype(F32)).astype(BF)
    g_row = lax.broadcasted_iota(jnp.int32, (32, 768), 0)
    g_lane = lax.broadcasted_iota(jnp.int32, (32, 768), 1)
    inside = (g_lane >= g_row * 24) & (g_lane < g_row * 24 + 24)
    place = jnp.where(inner_row == lane3, 1.0, 0.0).reshape(768, 128).astype(BF)
    packed = jnp.zeros((32, 128), F32)
    for part in (hi, mid, lo):
        spread_out = jnp.where(inside, part.astype(F32), 0.0).astype(BF)
        packed = packed + jnp.dot(spread_out, place, preferred_element_type=F32)
    k["rsc"][...] = packed.reshape(32, 1, 128)
    mine = me[Z] * 8 + me[X] * 2 + me[CORE]
    for t in spread(plane_offsets((Z, X, CORE))):
        there = coord(Z, t[Z]) * 8 + coord(X, t[X]) * 2 + coord(CORE, t[CORE])
        cp = remote(k["rsc"].at[there], k["rr"].at[mine, me[Y]], k["s_ret"], k["r_ret"], t)
        cp.start()
    k["rr"][mine, me[Y]] = k["rsc"][mine]
    k["hgs"][...] = (weight_row * k["acc"][...]).astype(BF)
    cp = pltpu.make_async_copy(k["hgs"], k["hg_h"], k["loc"].at[2 + NCH])
    cp.start()
    out_cps[NCH] = cp
    weight_grad(0)
    few = k["rsc"].at[pl.ds(0, 31)]
    pltpu.make_async_copy(few, few, k["r_ret"]).wait()
    column = k["rr"].at[:, me[Y]]
    y_cp = [
        launch(column, column, k["s_rety"].at[d - 1], k["r_rety"].at[d - 1], ring_offset(Y, d)) for d in (2, 1, 3)
    ]
    weight_grad(1)
    for cp in y_cp:
        cp.wait_recv()

    back = k["rr"][...].reshape(128, 128)
    mt = k["mt"][...]
    prob = k["prob"][...]
    score = jnp.zeros((128, 128), F32)
    for r in range(6):
        one = jnp.sum(jnp.where(t_col == 6 * me[Y] + r, back, 0.0), -1, keepdims=True)
        score = score + jnp.where(mt == float(r + 1), one, 0.0)
    grad_t = prob * (score - jnp.sum(prob * score, 0, keepdims=True))
    grad = grad_t.T

    def halves(v):
        top = v.astype(BF)
        return top, (v - top.astype(F32)).astype(BF)

    hi, lo = halves(grad)
    local = jnp.dot(k["normedt"][...], hi, preferred_element_type=F32) + jnp.dot(
        k["normedt"][...], lo, preferred_element_type=F32
    )
    hi, lo = halves(grad_t)
    normed_grad = jnp.dot(k["rw"][...], hi, preferred_element_type=F32) + jnp.dot(
        k["rw"][...], lo, preferred_element_type=F32
    )
    floated = k["res"][...].astype(F32)
    inv = lax.rsqrt(jnp.mean(floated * floated, 0, keepdims=True) + 1e-05)
    unit = floated * inv
    gain_col = jnp.sum(normed_grad * unit, -1, keepdims=True)
    k["gv"][...] = jnp.zeros_like(k["gv"])
    for j in range(23):
        n = min(128, D - 128 * j)
        col = gain_col[128 * j : 128 * j + n]
        k["gv"][j : j + 1, 0:n] = jnp.sum(jnp.where(eye[:n, :n], col, 0.0), 0, keepdims=True)
    xs = k["xs"]
    xs[pl.ds(0, 360)] = local.reshape(360, 8, 128).astype(BF)
    xs[pl.ds(360, 3)] = k["gv"][...].reshape(3, 8, 128).astype(BF)
    xs[pl.ds(363, 21)] = jnp.zeros((21, 8, 128), BF)

    a1 = []
    for n, (a, others) in enumerate(COLORS):
        for d in (2, 1, 3):
            piece = xs.at[pl.ds(pl.multiple_of(128 * n + 32 * coord(a, d), 32), 32)]
            a1.append(launch(piece, k["ar1"].at[n, d - 1], k["s_a1"].at[n, d - 1], k["r_a1"].at[n, d - 1], ring_offset(a, d)))
    upper = normed_grad * k["gc"][...]
    k["rg"][...] = (inv * (upper - unit * jnp.mean(upper * unit, 0, keepdims=True))).astype(BF)
    weight_grad(2)

    for n, (a, others) in enumerate(COLORS):
        for cp in a1[3 * n : 3 * n + 3]:
            cp.wait_recv()
        total = xs[pl.ds(pl.multiple_of(128 * n + 32 * me[a], 32), 32)].astype(F32)
        for d in range(3):
            total = total + k["ar1"][n, d].astype(F32)
        k["as2"][n] = total.astype(BF)
        ring = (SZ[others[1]] * SZ[others[2]], SZ[others[2]], 1)

        def rank(t):
            return sum(coord(o, t[o]) * s for o, s in zip(others, ring))

        here = rank((0, 0, 0, 0))
        for t in spread(plane_offsets(others)):
            cp = remote(k["as2"].at[n, rank(t)], k["ar2"].at[n, here], k["s_a2"].at[n], k["r_a2"].at[n], t)
            cp.start()
        k["ar2"][n, here] = k["as2"][n, here]
    weight_grad(3)
    tot = k["tot"]
    for n, (a, others) in enumerate(COLORS):
        few = k["as2"].at[n, pl.ds(0, 31)]
        pltpu.make_async_copy(few, few, k["r_a2"].at[n]).wait()
        ring = (SZ[others[1]] * SZ[others[2]], SZ[others[2]], 1)
        here = sum(me[o] * s for o, s in zip(others, ring))
        done = jnp.sum(k["ar2"][n].astype(F32), 0)
        at = 128 * n + 32 * me[a] + here
        tot[at] = done.astype(BF)
        for t in spread(plane_offsets(others)):
            cp = remote(tot.at[at], tot.at[at], k["s_g2"].at[n], k["r_g2"].at[n], t)
            cp.start()
    weight_grad(4)
    g1 = []
    for n, (a, others) in enumerate(COLORS):
        few = k["as2"].at[n, pl.ds(0, 31)]
        pltpu.make_async_copy(few, few, k["r_g2"].at[n]).wait()
        piece = tot.at[pl.ds(pl.multiple_of(128 * n + 32 * me[a], 32), 32)]
        for d in (2, 1, 3):
            g1.append(launch(piece, piece, k["s_g1"].at[n, d - 1], k["r_g1"].at[n, d - 1], ring_offset(a, d)))
    weight_grad(5)
    for cp in g1:
        cp.wait_recv()
    for cp in pending:
        cp.wait_send()
    few = k["rsc"].at[pl.ds(0, 31)]
    pltpu.make_async_copy(few, few, k["s_ret"]).wait()
    for n in range(3):
        few = k["as2"].at[n, pl.ds(0, 31)]
        pltpu.make_async_copy(few, few, k["s_a2"].at[n]).wait()
        pltpu.make_async_copy(few, few, k["s_g2"].at[n]).wait()
    for i, cp in out_cps.items():
        if i not in REUSE.values():
            cp.wait()


def finish(hg, wg, rg, tot, hg_o, wg_o, rg_o, router, gain, hg_v, wg_v, rg_v, tot_v, ro_v, rsem, wsem):
    parts = [(tot, tot_v, None)]
    for src, via, dst, rows in ((wg, wg_v, wg_o, 240), (hg, hg_v, hg_o, 480), (rg, rg_v, rg_o, 1440)):
        for r in range(0, src.shape[0], rows):
            at = pl.ds(r, rows)
            parts.append((src.at[at], via.at[at], dst.at[at]))
    reads = [pltpu.make_async_copy(s, v, rsem.at[n]) for n, (s, v, d) in enumerate(parts)]
    for cp in reads:
        cp.start()
    writes = []
    for n, (s, v, d) in enumerate(parts):
        reads[n].wait()
        if d is None:
            ro_v[...] = tot_v[pl.ds(0, 360)].astype(F32).reshape(D, 128)
            cp = pltpu.make_async_copy(ro_v, router, wsem.at[n])
            cp.start()
            writes.append(cp)
            rows = tot_v[pl.ds(360, 3)].astype(F32).reshape(24, 128)
            for j in range(23):
                m = min(128, D - 128 * j)
                gain[pl.ds(128 * j, m)] = rows[j : j + 1, 0:m].reshape(m)
        else:
            cp = pltpu.make_async_copy(v, d, wsem.at[n])
            cp.start()
            writes.append(cp)
    for cp in writes:
        cp.wait()


def on_device(residual, norm_gain, router_weight, out_grad, expert_ids, hidden, down_weight):
    vm = pl.BlockSpec(memory_space=pltpu.VMEM)
    hbm = pl.BlockSpec(memory_space=pl.ANY)
    dma = pltpu.SemaphoreType.DMA
    scratch = [
        pltpu.VMEM((FF, 768), BF), pltpu.VMEM((FF, D), BF), pltpu.VMEM((FF, 768), F32), pltpu.VMEM((FF, 768), BF),
        pltpu.VMEM((128, 128), F32), pltpu.VMEM((128, 128), F32), pltpu.VMEM((D, 128), BF), pltpu.VMEM((D, 128), F32),
        pltpu.VMEM((32, 1, 128), F32), pltpu.VMEM((32, 4, 1, 128), F32),
        pltpu.VMEM((384, 8, 128), BF), pltpu.VMEM((3, 3, 32, 8, 128), BF), pltpu.VMEM((3, 32, 8, 128), BF),
        pltpu.VMEM((3, 32, 8, 128), BF), pltpu.VMEM((24, 128), F32), pltpu.VMEM((768, D), BF),
    ]
    scratch += [pltpu.VMEM((4, 128, 128), BF) for _ in GDIMS]
    scratch += [pltpu.VMEM((4, 128, 128), BF)]
    scratch += [pltpu.VMEM((768, 512), BF) for _ in GDIMS]
    scratch += [pltpu.VMEM((768, 128), BF) for _ in GDIMS]
    scratch += [pltpu.VMEM((768, 768), BF) for _ in range(2)]
    for i, (c0, nc, cw, a, p, q) in enumerate(PLAN):
        sizes = tuple(SZ[o] for o in OTHER[a])
        scratch += [
            pltpu.VMEM((cw, 512), BF), pltpu.VMEM(sizes + (3, 8, cw), BF),
            pltpu.VMEM((4,) + tuple(SZ[o] for o in OTHER[a] if o != p) + (3, 8, cw), BF),
            pltpu.VMEM(sizes + (3, 8, cw), BF),
        ]
        if i not in REUSE:
            scratch.append(pltpu.VMEM((FF, nc), BF))
    ng = len(GDIMS)
    scratch += [dma((ng, 3)), dma((ng, 3)), dma((3,)), dma((3,)), dma((NCH, 3)), dma((NCH, 3))]
    scratch += [dma((NCH, 3)), dma((NCH, 3)), dma((NCH, 7)), dma((NCH, 7))]
    scratch += [dma(()), dma(()), dma((3,)), dma((3,)), dma((3, 3)), dma((3, 3)), dma((3,)), dma((3,))]
    scratch += [dma((3,)), dma((3,)), dma((3, 3)), dma((3, 3)), dma((3 + NCH,))]
    hidden_grad, weight_grad, residual_grad, total = pl.pallas_call(
        kernel,
        name="routed",
        out_shape=(
            jax.ShapeDtypeStruct((FF, 768), BF),
            jax.ShapeDtypeStruct((FF, D), BF),
            jax.ShapeDtypeStruct((D, 128), BF),
            jax.ShapeDtypeStruct((384, 8, 128), BF),
        ),
        in_specs=[vm, vm, vm, vm, vm, hbm, hbm],
        out_specs=(hbm, hbm, vm, vm),
        scratch_shapes=scratch,
        compiler_params=pltpu.CompilerParams(
            collective_id=0, has_side_effects=True, vmem_limit_bytes=67043328
        ),
    )(out_grad.T, residual.T, norm_gain, router_weight, expert_ids.T, hidden[0].T, down_weight[0])
    nparts = 1 + FF // 240 + FF // 480 + D // 1440
    hidden_grad, weight_grad, residual_grad, router_grad, gain_grad = pl.pallas_call(
        finish,
        name="finish",
        out_shape=(
            jax.ShapeDtypeStruct((FF, 768), BF),
            jax.ShapeDtypeStruct((FF, D), BF),
            jax.ShapeDtypeStruct((D, 128), BF),
            jax.ShapeDtypeStruct((D, 128), F32),
            jax.ShapeDtypeStruct((D,), F32),
        ),
        in_specs=[hbm, hbm, hbm, hbm],
        out_specs=(hbm, hbm, hbm, hbm, vm),
        scratch_shapes=[
            pltpu.VMEM((FF, 768), BF), pltpu.VMEM((FF, D), BF), pltpu.VMEM((D, 128), BF),
            pltpu.VMEM((384, 8, 128), BF), pltpu.VMEM((D, 128), F32), dma((nparts,)), dma((nparts,)),
        ],
        compiler_params=pltpu.CompilerParams(vmem_limit_bytes=67043328),
    )(hidden_grad, weight_grad, residual_grad, total)
    return hidden_grad.T[None], weight_grad[None], residual_grad.T, router_grad, gain_grad


def solution(mesh):
    finer = Mesh(mesh.devices.reshape(4, 4, 2, mesh.shape["dp"]), AX)
    rows = P(AX, None)
    cube = P(AX, None, None)
    return jax.shard_map(
        on_device,
        mesh=finer,
        in_specs=(rows, P(), P(), rows, rows, cube, cube),
        out_specs=(cube, cube, rows, P(), P()),
        check_vma=False,
    )
```

```python
import functools

import jax
import jax.numpy as jnp
from jax import lax
from jax.experimental import pallas as pl
from jax.experimental.pallas import tpu as pltpu
from jax.sharding import Mesh
from jax.sharding import PartitionSpec as P

AX = ("ep_0", "ep_1", "ep_2", "dp")
SZ = (4, 4, 2, 4)
Z, X, CORE, Y = 0, 1, 2, 3
STRIDE = (32, 8, 4, 1)
MESH = pl.DeviceIdType.MESH
D = 2880
FF = 1440
BF = jnp.bfloat16
F32 = jnp.float32

PLAN = (
    (0, 384, 384, Y, Z, X),
    (384, 384, 384, Z, X, Y),
    (768, 384, 384, X, Y, Z),
    (1152, 384, 384, Y, X, Z),
    (1536, 384, 384, Z, Y, X),
    (1920, 384, 384, X, Z, Y),
    (2304, 256, 256, Y, Z, X),
    (2560, 256, 256, Z, X, Y),
    (2816, 64, 128, X, Y, Z),
)
NCH = len(PLAN)
LAST = NCH - 1
PARTS = (0, 1152, 2304, 2880)
OUT_COLS = ((0, 768), (768, 768), (1536, 768), (2304, 576))
GDIMS = tuple(dict.fromkeys(c[3] for c in PLAN))
FB = 480
NT = (((1,), (1,)), ((), ()))
TN = (((0,), (0,)), ((), ()))
COLORS = ((Z, (X, CORE, Y)), (X, (Z, CORE, Y)), (Y, (Z, X, CORE)))
OTHER = {Z: (X, CORE, Y), X: (Z, CORE, Y), Y: (Z, X, CORE)}


def plane_offsets(dims):
    out = []
    for a in range(SZ[dims[0]]):
        for b in range(SZ[dims[1]]):
            for c in range(SZ[dims[2]]):
                if (a, b, c) != (0, 0, 0):
                    t = [0, 0, 0, 0]
                    t[dims[0]], t[dims[1]], t[dims[2]] = a, b, c
                    out.append(tuple(t))
    return out


def spread(offsets):
    def hops(t):
        return sum(min(t[i], SZ[i] - t[i]) for i in (Z, X, Y))

    return sorted(offsets, key=lambda t: -hops(t))


def ring_offset(dim, d):
    t = [0, 0, 0, 0]
    t[dim] = d
    return tuple(t)


PEERS = [
    (z, x, c, y)
    for z in range(4) for x in range(4) for c in range(2) for y in range(4)
    if (z, x, c, y) != (0, 0, 0, 0)
]


def kernel(*refs):
    names = (
        ["og", "res", "gain", "rw", "ids", "hid_h", "w_h"]
        + ["hg_h", "wg_h", "rg", "tot"]
        + ["hid", "w", "acc", "hgs", "mt", "prob", "normedt", "gc"]
        + ["rsc", "rr", "xs", "ar1", "as2", "ar2", "gv", "rows", "wgs0", "wgs1", "wgs3"]
    )
    ng = len(GDIMS)
    names += [f"mg{g}" for g in range(ng)] + ["pg"] + [f"pb{g}" for g in range(ng)]
    names += [f"pick{g}" for g in range(ng)]
    names += [f"perm{a}" for a in (Z, X)]
    for i in range(NCH):
        names += [f"tok{i}", f"sel{i}", f"b1_{i}", f"fin{i}"]
    names += ["s_m", "r_m", "s_p", "r_p", "s_ag", "r_ag", "s_p1", "r_p1", "s_p2", "r_p2"]
    names += ["s_ret", "r_ret", "s_a1", "r_a1", "s_a2", "r_a2"]
    names += ["s_g2", "r_g2", "s_g1", "r_g1", "loc"]
    assert len(names) == len(refs)
    k = dict(zip(names, refs))
    me = [lax.axis_index(a) for a in AX]

    def dev(t):
        return tuple(
            lax.rem(me[i] + t[i], SZ[i]) if t[i] else me[i] for i in range(4)
        )

    def coord(dim, d):
        return lax.rem(me[dim] + d, SZ[dim]) if d else me[dim]

    def remote(src, dst, ssem, rsem, t):
        return pltpu.make_async_remote_copy(
            src_ref=src, dst_ref=dst, send_sem=ssem, recv_sem=rsem,
            device_id=dev(t), device_id_type=MESH,
        )

    pending = []

    def launch(src, dst, ssem, rsem, t):
        cp = remote(src, dst, ssem, rsem, t)
        cp.start()
        pending.append(cp)
        return cp

    barrier = pltpu.get_barrier_semaphore()
    for t in PEERS:
        pl.semaphore_signal(barrier, inc=1, device_id=dev(t), device_id_type=MESH)
    w_copy = pltpu.make_async_copy(k["w_h"], k["w"], k["loc"].at[0])
    w_copy.start()
    hid_copy = pltpu.make_async_copy(k["hid_h"], k["hid"], k["loc"].at[1])
    hid_copy.start()

    e_row = lax.broadcasted_iota(jnp.int32, (128, 128), 0)
    t_col = lax.broadcasted_iota(jnp.int32, (128, 128), 1)
    match = e_row == k["ids"][0:1, :]
    for j in range(1, 4):
        match = match | (e_row == k["ids"][j : j + 1, :])
    matchf = match.astype(F32)
    earlier = jnp.where(e_row < t_col, 1.0, 0.0).astype(BF)
    count = jnp.dot(matchf.astype(BF), earlier, preferred_element_type=F32)
    mt = matchf * (count + 1.0)
    k["mt"][...] = mt
    for g, a in enumerate(GDIMS):
        k[f"mg{g}"][me[a]] = mt.astype(BF)
    nl, cl = PLAN[LAST][1:3]
    k[f"tok{LAST}"][nl:cl, :] = jnp.zeros((cl - nl, 512), BF)

    group = lax.broadcasted_iota(jnp.int32, (32, 24, 128), 0)
    inner_row = lax.broadcasted_iota(jnp.int32, (32, 24, 128), 1)
    lane3 = lax.broadcasted_iota(jnp.int32, (32, 24, 128), 2)
    src_of = (
        jnp.where(inner_row >= 6, 1, 0) + jnp.where(inner_row >= 12, 1, 0) + jnp.where(inner_row >= 18, 1, 0)
    )
    want = (inner_row - 6 * src_of + 1).astype(F32).reshape(768, 128)
    src_flat = src_of.reshape(768, 128)
    for g, a in enumerate(GDIMS):
        o = OTHER[a]
        n1, n2 = SZ[o[1]] * SZ[o[2]], SZ[o[2]]
        expert = STRIDE[a] * me[a] + STRIDE[o[0]] * (group // n1)
        expert = expert + STRIDE[o[1]] * ((group // n2) % SZ[o[1]]) + STRIDE[o[2]] * (group % n2)
        k[f"pick{g}"][...] = jnp.where(expert == lane3, 1.0, 0.0).reshape(768, 128).astype(BF)
    eye = e_row == t_col
    for j in range(23):
        n = min(128, D - 128 * j)
        row = k["gain"][pl.ds(128 * j, n)].reshape(1, n)
        col = jnp.sum(jnp.where(eye[:n, :n], row, 0.0), -1, keepdims=True)
        k["gc"][128 * j : 128 * j + n, :] = jnp.broadcast_to(col, (n, 128))
    pl.semaphore_wait(barrier, len(PEERS))

    m_cp = []
    for g, a in enumerate(GDIMS):
        own = k[f"mg{g}"].at[me[a]]
        m_cp.append([
            launch(own, own, k["s_m"].at[g, d - 1], k["r_m"].at[g, d - 1], ring_offset(a, d))
            for d in (2, 1, 3)
        ])
    ag = [[] for _ in PLAN]

    def gather(i, ds):
        c0, nc, cw, a, p, q = PLAN[i]
        src = k["og"].at[pl.ds(c0, nc)]
        dst = k[f"tok{i}"].at[pl.ds(0, nc), pl.ds(pl.multiple_of(me[a] * 128, 128), 128)]
        for d in ds:
            ag[i].append(
                launch(src, dst, k["s_ag"].at[i, d - 1], k["r_ag"].at[i, d - 1], ring_offset(a, d))
            )

    for i in range(NCH):
        gather(i, (2, 1, 3))
    for i, (c0, nc, cw, a, p, q) in enumerate(PLAN):
        k[f"tok{i}"][0:nc, pl.ds(pl.multiple_of(me[a] * 128, 128), 128)] = k["og"][c0 : c0 + nc, :]

    floated = k["res"][...].astype(F32)
    inv = lax.rsqrt(jnp.mean(floated * floated, 0, keepdims=True) + 1e-05)
    normed = (floated * inv * k["gc"][...]).astype(BF)
    k["normedt"][...] = normed
    logits = lax.dot_general(k["rw"][...], normed, TN, preferred_element_type=F32)
    expo = jnp.where(match, jnp.exp(logits), 0.0)
    prob = expo / jnp.sum(expo, 0, keepdims=True)
    k["prob"][...] = prob
    pa = PLAN[LAST][3]
    k["pg"][me[pa]] = prob.astype(BF)
    own = k["pg"].at[me[pa]]
    p_cp = [
        launch(own, own, k["s_p"].at[d - 1], k["r_p"].at[d - 1], ring_offset(pa, d)) for d in (2, 1, 3)
    ]

    p1 = {}

    def first_ring(i):
        c0, nc, cw, a, p, q = PLAN[i]
        g = GDIMS.index(a)
        pb = k[f"pb{g}"]
        if i < len(GDIMS):
            for cp in m_cp[g]:
                cp.wait_recv()
            for s in range(4):
                marks = jnp.dot(k[f"pick{g}"][...], k[f"mg{g}"][s], preferred_element_type=F32)
                hit = (marks == want) & (src_flat == s)
                pb[:, s * 128 : (s + 1) * 128] = jnp.where(hit, 1.0, 0.0).astype(BF)
        for cp in ag[i]:
            cp.wait_recv()
        rows = lax.dot_general(pb[...], k[f"tok{i}"][...], NT, preferred_element_type=F32)
        if i == LAST:
            for cp in p_cp:
                cp.wait_recv()
            sent = jnp.zeros((768, 128), F32)
            for s in range(4):
                weights = jnp.dot(k[f"pick{g}"][...], k["pg"][s], preferred_element_type=F32)
                sent = sent + pb[:, s * 128 : (s + 1) * 128].astype(F32) * weights
            sent = jnp.sum(sent, -1, keepdims=True)
            lane = lax.broadcasted_iota(jnp.int32, (768, cw), 1)
            rows = jnp.where(lane >= nc, sent, rows)
        others = OTHER[a]
        sel, b1 = k[f"sel{i}"], k[f"b1_{i}"]
        sel[...] = rows.reshape(tuple(SZ[o] for o in others) + (3, 8, cw)).astype(BF)
        cps = []
        for d in (2, 1, 3):
            spot = tuple(coord(p, d) if o == p else slice(None) for o in others)
            cps.append(launch(sel.at[spot], b1.at[me[p]], k["s_p1"].at[i, d - 1], k["r_p1"].at[i, d - 1], ring_offset(p, d)))
        p1[i] = cps
        b1[me[p]] = sel[tuple(me[p] if o == p else slice(None) for o in others)]

    for i in range(6):
        first_ring(i)

    slot = lax.broadcasted_iota(jnp.int32, (768, 128), 0)
    lane = lax.broadcasted_iota(jnp.int32, (768, 128), 1)
    src = (slot * 10923) // 65536
    rest = slot - 6 * src
    from_z = (src % 32) * 24 + (src // 32) * 6 + rest
    from_x = ((src // 32) * 8 + src % 8) * 24 + ((src // 8) % 4) * 6 + rest
    for a, origin in ((Z, from_z), (X, from_x)):
        for j in range(6):
            k[f"perm{a}"][:, 128 * j : 128 * j + 128] = jnp.where(origin == lane + 128 * j, 1.0, 0.0).astype(BF)
    w_copy.wait()
    hid_copy.wait()

    p2 = {}

    def second_ring(i):
        c0, nc, cw, a, p, q = PLAN[i]
        for cp in p1[i]:
            cp.wait_recv()
        others = OTHER[a]
        left = tuple(o for o in others if o != p)
        spot = tuple(slice(None) if o == p else me[o] for o in others)
        b1, fin = k[f"b1_{i}"], k[f"fin{i}"]

        def part_of(dq, dc):
            return (slice(None),) + tuple(coord(q, dq) if o == q else coord(CORE, dc) for o in left)

        cps = []
        n = 0
        for dq in (2, 1, 3, 0):
            for dc in (0, 1):
                if dq == 0 and dc == 0:
                    continue
                t = [0, 0, 0, 0]
                t[q], t[CORE] = dq, dc
                cps.append(launch(b1.at[part_of(dq, dc)], fin.at[spot], k["s_p2"].at[i, n], k["r_p2"].at[i, n], tuple(t)))
                n += 1
        p2[i] = cps
        fin[spot] = b1[part_of(0, 0)]

    def arrived(i):
        c0, nc, cw, a, p, q = PLAN[i]
        for cp in p2[i]:
            cp.wait_recv()
        rows = k[f"fin{i}"][...].reshape(96, 8, cw).astype(F32).reshape(768, cw)
        if a != Y:
            rows = jnp.dot(k[f"perm{a}"][...], rows.astype(BF), preferred_element_type=F32)
        weight = None
        if i == LAST:
            spot = lax.broadcasted_iota(jnp.int32, (16, cw), 1)
            weight = rows[:, nc : nc + 1], lax.dot_general(
                jnp.where(spot == nc, 1.0, 0.0).astype(BF), rows.astype(BF), NT, preferred_element_type=F32
            )[0:1]
            rows = rows[:, :nc]
        k["rows"][:, c0 : c0 + nc] = rows.astype(BF)
        return weight

    def inner_part(h):
        cols = slice(PARTS[h], PARTS[h + 1])

        def step(n, carry):
            at = pl.ds(pl.multiple_of(n * FB, FB), FB)
            part = lax.dot_general(k["w"][at, cols], k["rows"][:, cols], NT, preferred_element_type=F32)
            if h == 0:
                k["acc"][at, :] = part
            else:
                k["acc"][at, :] += part
            return carry

        lax.fori_loop(0, FF // FB, step, 0)

    for i in (0, 1, 2):
        second_ring(i)
    for i in (6, 7, 8):
        first_ring(i)
    for i in (3, 4, 5):
        second_ring(i)
    for i in (0, 1, 2):
        arrived(i)
    inner_part(0)
    for i in (6, 7, 8):
        second_ring(i)
    for i in (3, 4, 5):
        arrived(i)
    inner_part(1)
    for i in (6, 7, 8):
        weight = arrived(i)
    weight_col, weight_row = weight
    inner_part(2)

    out_cps = {}

    def weight_grad(i):
        c0, nc = OUT_COLS[i]
        scaled = (weight_col * k["rows"][:, c0 : c0 + nc].astype(F32)).astype(BF)
        out = k[("wgs0", "wgs1", "wgs0", "wgs3")[i]]
        if i == 2:
            out_cps[0].wait()

        def step(n, carry):
            at = pl.ds(pl.multiple_of(n * FB, FB), FB)
            out[at, :] = jnp.dot(k["hid"][at, :], scaled, preferred_element_type=F32).astype(BF)
            return carry

        lax.fori_loop(0, FF // FB, step, 0)
        cp = pltpu.make_async_copy(out, k["wg_h"].at[:, pl.ds(c0, nc)], k["loc"].at[2 + i])
        cp.start()
        out_cps[i] = cp

    slot_score = jnp.sum(k["acc"][...] * k["hid"][...].astype(F32), 0, keepdims=True)
    hi = slot_score.astype(BF)
    left = slot_score - hi.astype(F32)
    mid = left.astype(BF)
    lo = (left - mid.astype(F32)).astype(BF)
    g_row = lax.broadcasted_iota(jnp.int32, (128, 768), 0)
    g_lane = lax.broadcasted_iota(jnp.int32, (128, 768), 1)
    inside = (g_lane >= g_row * 6) & (g_lane < g_row * 6 + 6)
    place = jnp.where(rest == lane, 1.0, 0.0).astype(BF)
    packed = jnp.zeros((128, 128), F32)
    for part in (hi, mid, lo):
        spread_out = jnp.where(inside, part.astype(F32), 0.0).astype(BF)
        packed = packed + jnp.dot(spread_out, place, preferred_element_type=F32)
    k["rsc"][...] = packed.reshape(128, 1, 128)
    mine = sum(me[o] * STRIDE[o] for o in range(4))
    for t in spread(PEERS):
        there = sum(coord(o, t[o]) * STRIDE[o] for o in range(4))
        remote(k["rsc"].at[there], k["rr"].at[mine], k["s_ret"], k["r_ret"], t).start()
    k["rr"][mine] = k["rsc"][mine]
    k["hgs"][...] = (weight_row * k["acc"][...]).astype(BF)
    cp = pltpu.make_async_copy(k["hgs"], k["hg_h"], k["loc"].at[6])
    cp.start()
    out_cps[4] = cp
    weight_grad(0)
    few = k["rsc"].at[pl.ds(0, 127)]
    pltpu.make_async_copy(few, few, k["r_ret"]).wait()

    back = k["rr"][...].reshape(128, 128)
    mt = k["mt"][...]
    prob = k["prob"][...]
    score = jnp.zeros((128, 128), F32)
    for r in range(6):
        score = score + jnp.where(mt == float(r + 1), back[:, r : r + 1], 0.0)
    grad_t = prob * (score - jnp.sum(prob * score, 0, keepdims=True))
    grad = grad_t.T

    def halves(v):
        top = v.astype(BF)
        return top, (v - top.astype(F32)).astype(BF)

    hi, lo = halves(grad)
    local = jnp.dot(k["normedt"][...], hi, preferred_element_type=F32) + jnp.dot(
        k["normedt"][...], lo, preferred_element_type=F32
    )
    hi, lo = halves(grad_t)
    normed_grad = jnp.dot(k["rw"][...], hi, preferred_element_type=F32) + jnp.dot(
        k["rw"][...], lo, preferred_element_type=F32
    )
    floated = k["res"][...].astype(F32)
    inv = lax.rsqrt(jnp.mean(floated * floated, 0, keepdims=True) + 1e-05)
    unit = floated * inv
    gain_col = jnp.sum(normed_grad * unit, -1, keepdims=True)
    k["gv"][...] = jnp.zeros_like(k["gv"])
    for j in range(23):
        n = min(128, D - 128 * j)
        col = gain_col[128 * j : 128 * j + n]
        k["gv"][j : j + 1, 0:n] = jnp.sum(jnp.where(eye[:n, :n], col, 0.0), 0, keepdims=True)
    xs = k["xs"]
    xs[pl.ds(0, 360)] = local.reshape(360, 8, 128).astype(BF)
    xs[pl.ds(360, 3)] = k["gv"][...].reshape(3, 8, 128).astype(BF)
    xs[pl.ds(363, 21)] = jnp.zeros((21, 8, 128), BF)

    a1 = []
    for n, (a, others) in enumerate(COLORS):
        for d in (2, 1, 3):
            piece = xs.at[pl.ds(pl.multiple_of(128 * n + 32 * coord(a, d), 32), 32)]
            a1.append(launch(piece, k["ar1"].at[n, d - 1], k["s_a1"].at[n, d - 1], k["r_a1"].at[n, d - 1], ring_offset(a, d)))
    upper = normed_grad * k["gc"][...]
    k["rg"][...] = (inv * (upper - unit * jnp.mean(upper * unit, 0, keepdims=True))).astype(BF)
    weight_grad(1)

    for n, (a, others) in enumerate(COLORS):
        for cp in a1[3 * n : 3 * n + 3]:
            cp.wait_recv()
        total = xs[pl.ds(pl.multiple_of(128 * n + 32 * me[a], 32), 32)].astype(F32)
        for d in range(3):
            total = total + k["ar1"][n, d].astype(F32)
        k["as2"][n] = total.astype(BF)
        ring = (SZ[others[1]] * SZ[others[2]], SZ[others[2]], 1)

        def rank(t):
            return sum(coord(o, t[o]) * s for o, s in zip(others, ring))

        here = rank((0, 0, 0, 0))
        for t in spread(plane_offsets(others)):
            cp = remote(k["as2"].at[n, rank(t)], k["ar2"].at[n, here], k["s_a2"].at[n], k["r_a2"].at[n], t)
            cp.start()
        k["ar2"][n, here] = k["as2"][n, here]
    weight_grad(2)
    tot = k["tot"]
    for n, (a, others) in enumerate(COLORS):
        few = k["as2"].at[n, pl.ds(0, 31)]
        pltpu.make_async_copy(few, few, k["r_a2"].at[n]).wait()
        ring = (SZ[others[1]] * SZ[others[2]], SZ[others[2]], 1)
        here = sum(me[o] * s for o, s in zip(others, ring))
        done = jnp.sum(k["ar2"][n].astype(F32), 0)
        at = 128 * n + 32 * me[a] + here
        tot[at] = done.astype(BF)
        for t in spread(plane_offsets(others)):
            cp = remote(tot.at[at], tot.at[at], k["s_g2"].at[n], k["r_g2"].at[n], t)
            cp.start()
    weight_grad(3)
    g1 = []
    for n, (a, others) in enumerate(COLORS):
        few = k["as2"].at[n, pl.ds(0, 31)]
        pltpu.make_async_copy(few, few, k["r_g2"].at[n]).wait()
        piece = tot.at[pl.ds(pl.multiple_of(128 * n + 32 * me[a], 32), 32)]
        for d in (2, 1, 3):
            g1.append(launch(piece, piece, k["s_g1"].at[n, d - 1], k["r_g1"].at[n, d - 1], ring_offset(a, d)))
    for cp in g1:
        cp.wait_recv()
    for cp in pending:
        cp.wait_send()
    few = k["rsc"].at[pl.ds(0, 127)]
    pltpu.make_async_copy(few, few, k["s_ret"]).wait()
    for n in range(3):
        few = k["as2"].at[n, pl.ds(0, 31)]
        pltpu.make_async_copy(few, few, k["s_a2"].at[n]).wait()
        pltpu.make_async_copy(few, few, k["s_g2"].at[n]).wait()
    for i, cp in out_cps.items():
        if i != 0:
            cp.wait()


def finish(hg, wg, rg, tot, hg_o, wg_o, rg_o, router, gain, hg_v, wg_v, rg_v, tot_v, ro_v, rsem, wsem):
    parts = [(tot, tot_v, None)]
    for src, via, dst, rows in ((wg, wg_v, wg_o, 240), (hg, hg_v, hg_o, 480), (rg, rg_v, rg_o, 1440)):
        for r in range(0, src.shape[0], rows):
            at = pl.ds(r, rows)
            parts.append((src.at[at], via.at[at], dst.at[at]))
    reads = [pltpu.make_async_copy(s, v, rsem.at[n]) for n, (s, v, d) in enumerate(parts)]
    for cp in reads:
        cp.start()
    writes = []
    for n, (s, v, d) in enumerate(parts):
        reads[n].wait()
        if d is None:
            ro_v[...] = tot_v[pl.ds(0, 360)].astype(F32).reshape(D, 128)
            cp = pltpu.make_async_copy(ro_v, router, wsem.at[n])
            cp.start()
            writes.append(cp)
            rows = tot_v[pl.ds(360, 3)].astype(F32).reshape(24, 128)
            for j in range(23):
                m = min(128, D - 128 * j)
                gain[pl.ds(128 * j, m)] = rows[j : j + 1, 0:m].reshape(m)
        else:
            cp = pltpu.make_async_copy(v, d, wsem.at[n])
            cp.start()
            writes.append(cp)
    for cp in writes:
        cp.wait()


def on_device(residual, norm_gain, router_weight, out_grad, expert_ids, hidden, down_weight):
    vm = pl.BlockSpec(memory_space=pltpu.VMEM)
    hbm = pl.BlockSpec(memory_space=pl.ANY)
    dma = pltpu.SemaphoreType.DMA
    scratch = [
        pltpu.VMEM((FF, 768), BF), pltpu.VMEM((FF, D), BF), pltpu.VMEM((FF, 768), F32), pltpu.VMEM((FF, 768), BF),
        pltpu.VMEM((128, 128), F32), pltpu.VMEM((128, 128), F32), pltpu.VMEM((D, 128), BF), pltpu.VMEM((D, 128), F32),
        pltpu.VMEM((128, 1, 128), F32), pltpu.VMEM((128, 1, 128), F32),
        pltpu.VMEM((384, 8, 128), BF), pltpu.VMEM((3, 3, 32, 8, 128), BF), pltpu.VMEM((3, 32, 8, 128), BF),
        pltpu.VMEM((3, 32, 8, 128), BF), pltpu.VMEM((24, 128), F32), pltpu.VMEM((768, D), BF),
        pltpu.VMEM((FF, 768), BF), pltpu.VMEM((FF, 768), BF), pltpu.VMEM((FF, 576), BF),
    ]
    scratch += [pltpu.VMEM((4, 128, 128), BF) for _ in GDIMS]
    scratch += [pltpu.VMEM((4, 128, 128), BF)]
    scratch += [pltpu.VMEM((768, 512), BF) for _ in GDIMS]
    scratch += [pltpu.VMEM((768, 128), BF) for _ in GDIMS]
    scratch += [pltpu.VMEM((768, 768), BF) for _ in range(2)]
    for i, (c0, nc, cw, a, p, q) in enumerate(PLAN):
        sizes = tuple(SZ[o] for o in OTHER[a])
        scratch += [
            pltpu.VMEM((cw, 512), BF), pltpu.VMEM(sizes + (3, 8, cw), BF),
            pltpu.VMEM((4,) + tuple(SZ[o] for o in OTHER[a] if o != p) + (3, 8, cw), BF),
            pltpu.VMEM(sizes + (3, 8, cw), BF),
        ]
    ng = len(GDIMS)
    scratch += [dma((ng, 3)), dma((ng, 3)), dma((3,)), dma((3,)), dma((NCH, 3)), dma((NCH, 3))]
    scratch += [dma((NCH, 3)), dma((NCH, 3)), dma((NCH, 7)), dma((NCH, 7))]
    scratch += [dma(()), dma(()), dma((3, 3)), dma((3, 3)), dma((3,)), dma((3,))]
    scratch += [dma((3,)), dma((3,)), dma((3, 3)), dma((3, 3)), dma((7,))]
    hidden_grad, weight_grad, residual_grad, total = pl.pallas_call(
        kernel,
        name="routed",
        out_shape=(
            jax.ShapeDtypeStruct((FF, 768), BF),
            jax.ShapeDtypeStruct((FF, D), BF),
            jax.ShapeDtypeStruct((D, 128), BF),
            jax.ShapeDtypeStruct((384, 8, 128), BF),
        ),
        in_specs=[vm, vm, vm, vm, vm, hbm, hbm],
        out_specs=(hbm, hbm, vm, vm),
        scratch_shapes=scratch,
        compiler_params=pltpu.CompilerParams(
            collective_id=0, has_side_effects=True, vmem_limit_bytes=67043328
        ),
    )(out_grad.T, residual.T, norm_gain, router_weight, expert_ids.T, hidden[0].T, down_weight[0])
    nparts = 1 + FF // 240 + FF // 480 + D // 1440
    hidden_grad, weight_grad, residual_grad, router_grad, gain_grad = pl.pallas_call(
        finish,
        name="finish",
        out_shape=(
            jax.ShapeDtypeStruct((FF, 768), BF),
            jax.ShapeDtypeStruct((FF, D), BF),
            jax.ShapeDtypeStruct((D, 128), BF),
            jax.ShapeDtypeStruct((D, 128), F32),
            jax.ShapeDtypeStruct((D,), F32),
        ),
        in_specs=[hbm, hbm, hbm, hbm],
        out_specs=(hbm, hbm, hbm, hbm, vm),
        scratch_shapes=[
            pltpu.VMEM((FF, 768), BF), pltpu.VMEM((FF, D), BF), pltpu.VMEM((D, 128), BF),
            pltpu.VMEM((384, 8, 128), BF), pltpu.VMEM((D, 128), F32), dma((nparts,)), dma((nparts,)),
        ],
        compiler_params=pltpu.CompilerParams(vmem_limit_bytes=67043328),
    )(hidden_grad, weight_grad, residual_grad, total)
    return hidden_grad.T[None], weight_grad[None], residual_grad.T, router_grad, gain_grad


def solution(mesh):
    finer = Mesh(mesh.devices.reshape(4, 4, 2, mesh.shape["dp"]), AX)
    rows = P(AX, None)
    cube = P(AX, None, None)
    return jax.shard_map(
        on_device,
        mesh=finer,
        in_specs=(rows, P(), P(), rows, rows, cube, cube),
        out_specs=(cube, cube, rows, P(), P()),
        check_vma=False,
    )
```

```python
import functools

import jax
import jax.numpy as jnp
from jax import lax
from jax.experimental import pallas as pl
from jax.experimental.pallas import tpu as pltpu
from jax.sharding import Mesh
from jax.sharding import PartitionSpec as P

AX = ("ep_0", "ep_1", "ep_2", "dp")
SZ = (4, 4, 2, 4)
Z, X, CORE, Y = 0, 1, 2, 3
STRIDE = (32, 8, 4, 1)
MESH = pl.DeviceIdType.MESH
D = 2880
FF = 1440
BF = jnp.bfloat16
F32 = jnp.float32

PLAN = (
    (0, 512, 512, Y, Z, X),
    (512, 512, 512, Z, X, Y),
    (1024, 512, 512, X, Y, Z),
    (1536, 256, 256, Y, X, Z),
    (1792, 256, 256, Z, Y, X),
    (2048, 256, 256, X, Z, Y),
    (2304, 256, 256, Y, Z, X),
    (2560, 256, 256, Z, X, Y),
    (2816, 64, 128, X, Y, Z),
)
NCH = len(PLAN)
LAST = NCH - 1
PARTS = (0, 1536, 2304, 2880)
OUT_COLS = ((0, 768), (768, 768), (1536, 768), (2304, 576))
GDIMS = tuple(dict.fromkeys(c[3] for c in PLAN))
FB = 480
NT = (((1,), (1,)), ((), ()))
TN = (((0,), (0,)), ((), ()))
COLORS = ((Z, (X, CORE, Y)), (X, (Z, CORE, Y)), (Y, (Z, X, CORE)))
OTHER = {Z: (X, CORE, Y), X: (Z, CORE, Y), Y: (Z, X, CORE)}


def plane_offsets(dims):
    out = []
    for a in range(SZ[dims[0]]):
        for b in range(SZ[dims[1]]):
            for c in range(SZ[dims[2]]):
                if (a, b, c) != (0, 0, 0):
                    t = [0, 0, 0, 0]
                    t[dims[0]], t[dims[1]], t[dims[2]] = a, b, c
                    out.append(tuple(t))
    return out


def spread(offsets):
    def hops(t):
        return sum(min(t[i], SZ[i] - t[i]) for i in (Z, X, Y))

    return sorted(offsets, key=lambda t: -hops(t))


def ring_offset(dim, d):
    t = [0, 0, 0, 0]
    t[dim] = d
    return tuple(t)


PEERS = [
    (z, x, c, y)
    for z in range(4) for x in range(4) for c in range(2) for y in range(4)
    if (z, x, c, y) != (0, 0, 0, 0)
]


def kernel(*refs):
    names = (
        ["og_h", "res_h", "gain_h", "rw_h", "ids_h", "hid_h", "w_h"]
        + ["hg_h", "wg_h", "rg_h", "tot_h"]
        + ["og", "res", "gain", "rw", "ids", "rg", "tot", "hid", "w", "acc", "hgs", "mt", "prob", "normedt", "gc"]
        + ["rsc", "rr", "xs", "ar1", "as2", "ar2", "gv", "rows", "wgs0", "wgs1", "wgs3"]
    )
    ng = len(GDIMS)
    names += [f"mg{g}" for g in range(ng)] + ["pg"] + [f"pb{g}" for g in range(ng)]
    names += [f"pick{g}" for g in range(ng)]
    names += [f"perm{a}" for a in (Z, X)]
    for i in range(NCH):
        names += [f"tok{i}", f"sel{i}", f"b1_{i}", f"fin{i}"]
    names += ["s_m", "r_m", "s_p", "r_p", "s_ag", "r_ag", "s_p1", "r_p1", "s_p2", "r_p2"]
    names += ["s_ret", "r_ret", "s_a1", "r_a1", "s_a2", "r_a2"]
    names += ["s_g2", "r_g2", "s_g1", "r_g1", "loc"]
    assert len(names) == len(refs)
    k = dict(zip(names, refs))
    me = [lax.axis_index(a) for a in AX]

    def dev(t):
        return tuple(
            lax.rem(me[i] + t[i], SZ[i]) if t[i] else me[i] for i in range(4)
        )

    def coord(dim, d):
        return lax.rem(me[dim] + d, SZ[dim]) if d else me[dim]

    def remote(src, dst, ssem, rsem, t):
        return pltpu.make_async_remote_copy(
            src_ref=src, dst_ref=dst, send_sem=ssem, recv_sem=rsem,
            device_id=dev(t), device_id_type=MESH,
        )

    pending = []

    def launch(src, dst, ssem, rsem, t):
        cp = remote(src, dst, ssem, rsem, t)
        cp.start()
        pending.append(cp)
        return cp

    fetch = {}
    for n, name in enumerate(("ids", "gain", "og", "res", "rw")):
        fetch[name] = pltpu.make_async_copy(k[name + "_h"], k[name], k["loc"].at[7 + n])
        fetch[name].start()
    barrier = pltpu.get_barrier_semaphore()
    for t in PEERS:
        pl.semaphore_signal(barrier, inc=1, device_id=dev(t), device_id_type=MESH)
    w_copy = pltpu.make_async_copy(k["w_h"], k["w"], k["loc"].at[0])
    w_copy.start()
    hid_copy = pltpu.make_async_copy(k["hid_h"], k["hid"], k["loc"].at[1])
    hid_copy.start()

    e_row = lax.broadcasted_iota(jnp.int32, (128, 128), 0)
    t_col = lax.broadcasted_iota(jnp.int32, (128, 128), 1)
    fetch["ids"].wait()
    match = e_row == k["ids"][0:1, :]
    for j in range(1, 4):
        match = match | (e_row == k["ids"][j : j + 1, :])
    matchf = match.astype(F32)
    earlier = jnp.where(e_row < t_col, 1.0, 0.0).astype(BF)
    count = jnp.dot(matchf.astype(BF), earlier, preferred_element_type=F32)
    mt = matchf * (count + 1.0)
    k["mt"][...] = mt
    for g, a in enumerate(GDIMS):
        k[f"mg{g}"][me[a]] = mt.astype(BF)
    nl, cl = PLAN[LAST][1:3]
    k[f"tok{LAST}"][nl:cl, :] = jnp.zeros((cl - nl, 512), BF)

    group = lax.broadcasted_iota(jnp.int32, (32, 24, 128), 0)
    inner_row = lax.broadcasted_iota(jnp.int32, (32, 24, 128), 1)
    lane3 = lax.broadcasted_iota(jnp.int32, (32, 24, 128), 2)
    src_of = (
        jnp.where(inner_row >= 6, 1, 0) + jnp.where(inner_row >= 12, 1, 0) + jnp.where(inner_row >= 18, 1, 0)
    )
    want = (inner_row - 6 * src_of + 1).astype(F32).reshape(768, 128)
    src_flat = src_of.reshape(768, 128)
    for g, a in enumerate(GDIMS):
        o = OTHER[a]
        n1, n2 = SZ[o[1]] * SZ[o[2]], SZ[o[2]]
        expert = STRIDE[a] * me[a] + STRIDE[o[0]] * (group // n1)
        expert = expert + STRIDE[o[1]] * ((group // n2) % SZ[o[1]]) + STRIDE[o[2]] * (group % n2)
        k[f"pick{g}"][...] = jnp.where(expert == lane3, 1.0, 0.0).reshape(768, 128).astype(BF)
    eye = e_row == t_col
    fetch["gain"].wait()
    for j in range(23):
        n = min(128, D - 128 * j)
        row = k["gain"][pl.ds(128 * j, n)].reshape(1, n)
        col = jnp.sum(jnp.where(eye[:n, :n], row, 0.0), -1, keepdims=True)
        k["gc"][128 * j : 128 * j + n, :] = jnp.broadcast_to(col, (n, 128))
    fetch["og"].wait()
    pl.semaphore_wait(barrier, len(PEERS))

    m_cp = []
    for g, a in enumerate(GDIMS):
        own = k[f"mg{g}"].at[me[a]]
        m_cp.append([
            launch(own, own, k["s_m"].at[g, d - 1], k["r_m"].at[g, d - 1], ring_offset(a, d))
            for d in (2, 1, 3)
        ])
    ag = [[] for _ in PLAN]

    def lanes_of(a, d):
        return pl.ds(pl.multiple_of(coord(a, d) * 128, 128), 128)

    def gather(i):
        c0, nc, cw, a, p, q = PLAN[i]
        src = k["og"].at[pl.ds(c0, nc)]
        dst = k[f"tok{i}"].at[pl.ds(0, nc), lanes_of(a, 0)]
        for n, d in enumerate((1, 3)):
            ag[i].append(launch(src, dst, k["s_ag"].at[i, n], k["r_ag"].at[i, n], ring_offset(a, d)))

    def relay(i):
        c0, nc, cw, a, p, q = PLAN[i]
        half = nc // 2
        for n, d in enumerate((1, 3)):
            ag[i][n].wait_recv()
            piece = k[f"tok{i}"].at[pl.ds(n * half, half), lanes_of(a, 4 - d)]
            ag[i].append(
                launch(piece, piece, k["s_ag"].at[i, 2 + n], k["r_ag"].at[i, 2 + n], ring_offset(a, d))
            )

    for i in range(NCH):
        gather(i)
    for i, (c0, nc, cw, a, p, q) in enumerate(PLAN):
        k[f"tok{i}"][0:nc, pl.ds(pl.multiple_of(me[a] * 128, 128), 128)] = k["og"][c0 : c0 + nc, :]

    fetch["res"].wait()
    fetch["rw"].wait()
    floated = k["res"][...].astype(F32)
    inv = lax.rsqrt(jnp.mean(floated * floated, 0, keepdims=True) + 1e-05)
    normed = (floated * inv * k["gc"][...]).astype(BF)
    k["normedt"][...] = normed
    logits = lax.dot_general(k["rw"][...], normed, TN, preferred_element_type=F32)
    expo = jnp.where(match, jnp.exp(logits), 0.0)
    prob = expo / jnp.sum(expo, 0, keepdims=True)
    k["prob"][...] = prob
    pa = PLAN[LAST][3]
    k["pg"][me[pa]] = prob.astype(BF)
    own = k["pg"].at[me[pa]]
    p_cp = [
        launch(own, own, k["s_p"].at[d - 1], k["r_p"].at[d - 1], ring_offset(pa, d)) for d in (2, 1, 3)
    ]

    p1 = {}

    def first_ring(i):
        c0, nc, cw, a, p, q = PLAN[i]
        g = GDIMS.index(a)
        pb = k[f"pb{g}"]
        if i < len(GDIMS):
            for cp in m_cp[g]:
                cp.wait_recv()
            for s in range(4):
                marks = jnp.dot(k[f"pick{g}"][...], k[f"mg{g}"][s], preferred_element_type=F32)
                hit = (marks == want) & (src_flat == s)
                pb[:, s * 128 : (s + 1) * 128] = jnp.where(hit, 1.0, 0.0).astype(BF)
        for cp in ag[i][2:]:
            cp.wait_recv()
        rows = lax.dot_general(pb[...], k[f"tok{i}"][...], NT, preferred_element_type=F32)
        if i == LAST:
            for cp in p_cp:
                cp.wait_recv()
            sent = jnp.zeros((768, 128), F32)
            for s in range(4):
                weights = jnp.dot(k[f"pick{g}"][...], k["pg"][s], preferred_element_type=F32)
                sent = sent + pb[:, s * 128 : (s + 1) * 128].astype(F32) * weights
            sent = jnp.sum(sent, -1, keepdims=True)
            lane = lax.broadcasted_iota(jnp.int32, (768, cw), 1)
            rows = jnp.where(lane >= nc, sent, rows)
        others = OTHER[a]
        sel, b1 = k[f"sel{i}"], k[f"b1_{i}"]
        sel[...] = rows.reshape(tuple(SZ[o] for o in others) + (3, 8, cw)).astype(BF)
        cps = []
        for d in (2, 1, 3):
            spot = tuple(coord(p, d) if o == p else slice(None) for o in others)
            cps.append(launch(sel.at[spot], b1.at[me[p]], k["s_p1"].at[i, d - 1], k["r_p1"].at[i, d - 1], ring_offset(p, d)))
        p1[i] = cps
        b1[me[p]] = sel[tuple(me[p] if o == p else slice(None) for o in others)]

    for i in range(6):
        relay(i)
    for i in (0, 1, 2):
        first_ring(i)
    for i in (6, 7, 8):
        relay(i)
    for i in (3, 4, 5):
        first_ring(i)

    slot = lax.broadcasted_iota(jnp.int32, (768, 128), 0)
    lane = lax.broadcasted_iota(jnp.int32, (768, 128), 1)
    src = (slot * 10923) // 65536
    rest = slot - 6 * src
    from_z = (src % 32) * 24 + (src // 32) * 6 + rest
    from_x = ((src // 32) * 8 + src % 8) * 24 + ((src // 8) % 4) * 6 + rest
    for a, origin in ((Z, from_z), (X, from_x)):
        for j in range(6):
            k[f"perm{a}"][:, 128 * j : 128 * j + 128] = jnp.where(origin == lane + 128 * j, 1.0, 0.0).astype(BF)
    w_copy.wait()
    hid_copy.wait()

    p2 = {}

    def second_ring(i):
        c0, nc, cw, a, p, q = PLAN[i]
        for cp in p1[i]:
            cp.wait_recv()
        others = OTHER[a]
        left = tuple(o for o in others if o != p)
        spot = tuple(slice(None) if o == p else me[o] for o in others)
        b1, fin = k[f"b1_{i}"], k[f"fin{i}"]

        def part_of(dq, dc):
            return (slice(None),) + tuple(coord(q, dq) if o == q else coord(CORE, dc) for o in left)

        cps = []
        n = 0
        for dq in (2, 1, 3, 0):
            for dc in (0, 1):
                if dq == 0 and dc == 0:
                    continue
                t = [0, 0, 0, 0]
                t[q], t[CORE] = dq, dc
                cps.append(launch(b1.at[part_of(dq, dc)], fin.at[spot], k["s_p2"].at[i, n], k["r_p2"].at[i, n], tuple(t)))
                n += 1
        p2[i] = cps
        fin[spot] = b1[part_of(0, 0)]

    def arrived(i):
        c0, nc, cw, a, p, q = PLAN[i]
        for cp in p2[i]:
            cp.wait_recv()
        rows = k[f"fin{i}"][...].reshape(96, 8, cw).astype(F32).reshape(768, cw)
        if a != Y:
            rows = jnp.dot(k[f"perm{a}"][...], rows.astype(BF), preferred_element_type=F32)
        weight = None
        if i == LAST:
            spot = lax.broadcasted_iota(jnp.int32, (16, cw), 1)
            weight = rows[:, nc : nc + 1], lax.dot_general(
                jnp.where(spot == nc, 1.0, 0.0).astype(BF), rows.astype(BF), NT, preferred_element_type=F32
            )[0:1]
            rows = rows[:, :nc]
        k["rows"][:, c0 : c0 + nc] = rows.astype(BF)
        return weight

    def inner_part(h, first=0, last=FF // FB):
        cols = slice(PARTS[h], PARTS[h + 1])

        def step(n, carry):
            at = pl.ds(pl.multiple_of(n * FB, FB), FB)
            part = lax.dot_general(k["w"][at, cols], k["rows"][:, cols], NT, preferred_element_type=F32)
            if h == 0:
                k["acc"][at, :] = part
            else:
                k["acc"][at, :] += part
            return carry

        lax.fori_loop(first, last, step, 0)

    for i in (0, 1, 2):
        second_ring(i)
    for i in (6, 7, 8):
        first_ring(i)
    for i in (3, 4, 5):
        second_ring(i)
    for i in (0, 1, 2):
        arrived(i)
    inner_part(0, 0, 2)
    for i in (6, 7, 8):
        second_ring(i)
    inner_part(0, 2, 3)
    for i in (3, 4, 5):
        arrived(i)
    inner_part(1)
    for i in (6, 7, 8):
        weight = arrived(i)
    weight_col, weight_row = weight
    inner_part(2)

    out_cps = {}

    def weight_grad(i):
        c0, nc = OUT_COLS[i]
        scaled = (weight_col * k["rows"][:, c0 : c0 + nc].astype(F32)).astype(BF)
        out = k[("wgs0", "wgs1", "wgs0", "wgs3")[i]]
        if i == 2:
            out_cps[0].wait()

        def step(n, carry):
            at = pl.ds(pl.multiple_of(n * FB, FB), FB)
            out[at, :] = jnp.dot(k["hid"][at, :], scaled, preferred_element_type=F32).astype(BF)
            return carry

        lax.fori_loop(0, FF // FB, step, 0)
        cp = pltpu.make_async_copy(out, k["wg_h"].at[:, pl.ds(c0, nc)], k["loc"].at[2 + i])
        cp.start()
        out_cps[i] = cp

    slot_score = jnp.sum(k["acc"][...] * k["hid"][...].astype(F32), 0, keepdims=True)
    hi = slot_score.astype(BF)
    lo = (slot_score - hi.astype(F32)).astype(BF)
    g_row = lax.broadcasted_iota(jnp.int32, (128, 768), 0)
    g_lane = lax.broadcasted_iota(jnp.int32, (128, 768), 1)
    inside = (g_lane >= g_row * 6) & (g_lane < g_row * 6 + 6)
    place = jnp.where(rest == lane, 1.0, 0.0).astype(BF)
    packed = jnp.zeros((128, 128), F32)
    for part in (hi, lo):
        spread_out = jnp.where(inside, part.astype(F32), 0.0).astype(BF)
        packed = packed + jnp.dot(spread_out, place, preferred_element_type=F32)
    k["rsc"][...] = packed.reshape(128, 1, 128)
    mine = sum(me[o] * STRIDE[o] for o in range(4))
    for t in spread(PEERS):
        there = sum(coord(o, t[o]) * STRIDE[o] for o in range(4))
        remote(k["rsc"].at[there], k["rr"].at[mine], k["s_ret"], k["r_ret"], t).start()
    k["rr"][mine] = k["rsc"][mine]
    k["hgs"][...] = (weight_row * k["acc"][...]).astype(BF)
    cp = pltpu.make_async_copy(k["hgs"], k["hg_h"], k["loc"].at[6])
    cp.start()
    out_cps[4] = cp
    weight_grad(0)
    few = k["rsc"].at[pl.ds(0, 127)]
    pltpu.make_async_copy(few, few, k["r_ret"]).wait()

    back = k["rr"][...].reshape(128, 128)
    mt = k["mt"][...]
    prob = k["prob"][...]
    score = jnp.zeros((128, 128), F32)
    for r in range(6):
        score = score + jnp.where(mt == float(r + 1), back[:, r : r + 1], 0.0)
    grad_t = prob * (score - jnp.sum(prob * score, 0, keepdims=True))
    grad = grad_t.T

    def halves(v):
        top = v.astype(BF)
        return top, (v - top.astype(F32)).astype(BF)

    hi, lo = halves(grad)
    local = jnp.dot(k["normedt"][...], hi, preferred_element_type=F32) + jnp.dot(
        k["normedt"][...], lo, preferred_element_type=F32
    )
    hi, lo = halves(grad_t)
    normed_grad = jnp.dot(k["rw"][...], hi, preferred_element_type=F32) + jnp.dot(
        k["rw"][...], lo, preferred_element_type=F32
    )
    floated = k["res"][...].astype(F32)
    inv = lax.rsqrt(jnp.mean(floated * floated, 0, keepdims=True) + 1e-05)
    unit = floated * inv
    gain_col = jnp.sum(normed_grad * unit, -1, keepdims=True)
    k["gv"][...] = jnp.zeros_like(k["gv"])
    for j in range(23):
        n = min(128, D - 128 * j)
        col = gain_col[128 * j : 128 * j + n]
        k["gv"][j : j + 1, 0:n] = jnp.sum(jnp.where(eye[:n, :n], col, 0.0), 0, keepdims=True)
    xs = k["xs"]
    xs[pl.ds(0, 360)] = local.reshape(360, 8, 128).astype(BF)
    xs[pl.ds(360, 3)] = k["gv"][...].reshape(3, 8, 128).astype(BF)
    xs[pl.ds(363, 21)] = jnp.zeros((21, 8, 128), BF)

    a1 = []
    for n, (a, others) in enumerate(COLORS):
        for d in (2, 1, 3):
            piece = xs.at[pl.ds(pl.multiple_of(128 * n + 32 * coord(a, d), 32), 32)]
            a1.append(launch(piece, k["ar1"].at[n, d - 1], k["s_a1"].at[n, d - 1], k["r_a1"].at[n, d - 1], ring_offset(a, d)))
    upper = normed_grad * k["gc"][...]
    k["rg"][...] = (inv * (upper - unit * jnp.mean(upper * unit, 0, keepdims=True))).astype(BF)
    cp = pltpu.make_async_copy(k["rg"], k["rg_h"], k["loc"].at[12])
    cp.start()
    out_cps[5] = cp
    weight_grad(1)

    for n, (a, others) in enumerate(COLORS):
        for cp in a1[3 * n : 3 * n + 3]:
            cp.wait_recv()
        total = xs[pl.ds(pl.multiple_of(128 * n + 32 * me[a], 32), 32)].astype(F32)
        for d in range(3):
            total = total + k["ar1"][n, d].astype(F32)
        k["as2"][n] = total.astype(BF)
        ring = (SZ[others[1]] * SZ[others[2]], SZ[others[2]], 1)

        def rank(t):
            return sum(coord(o, t[o]) * s for o, s in zip(others, ring))

        here = rank((0, 0, 0, 0))
        for t in spread(plane_offsets(others)):
            cp = remote(k["as2"].at[n, rank(t)], k["ar2"].at[n, here], k["s_a2"].at[n], k["r_a2"].at[n], t)
            cp.start()
        k["ar2"][n, here] = k["as2"][n, here]
    weight_grad(2)
    tot = k["tot"]
    for n, (a, others) in enumerate(COLORS):
        few = k["as2"].at[n, pl.ds(0, 31)]
        pltpu.make_async_copy(few, few, k["r_a2"].at[n]).wait()
        ring = (SZ[others[1]] * SZ[others[2]], SZ[others[2]], 1)
        here = sum(me[o] * s for o, s in zip(others, ring))
        done = jnp.sum(k["ar2"][n].astype(F32), 0)
        at = 128 * n + 32 * me[a] + here
        tot[at] = done.astype(BF)
        for t in spread(plane_offsets(others)):
            cp = remote(tot.at[at], tot.at[at], k["s_g2"].at[n], k["r_g2"].at[n], t)
            cp.start()
    weight_grad(3)
    g1 = []
    for n, (a, others) in enumerate(COLORS):
        few = k["as2"].at[n, pl.ds(0, 31)]
        pltpu.make_async_copy(few, few, k["r_g2"].at[n]).wait()
        piece = tot.at[pl.ds(pl.multiple_of(128 * n + 32 * me[a], 32), 32)]
        for d in (2, 1, 3):
            g1.append(launch(piece, piece, k["s_g1"].at[n, d - 1], k["r_g1"].at[n, d - 1], ring_offset(a, d)))
    for cp in g1:
        cp.wait_recv()
    cp = pltpu.make_async_copy(k["tot"], k["tot_h"], k["loc"].at[13])
    cp.start()
    out_cps[6] = cp
    for cp in pending:
        cp.wait_send()
    few = k["rsc"].at[pl.ds(0, 127)]
    pltpu.make_async_copy(few, few, k["s_ret"]).wait()
    for n in range(3):
        few = k["as2"].at[n, pl.ds(0, 31)]
        pltpu.make_async_copy(few, few, k["s_a2"].at[n]).wait()
        pltpu.make_async_copy(few, few, k["s_g2"].at[n]).wait()
    for i, cp in out_cps.items():
        if i != 0:
            cp.wait()


def finish(hg, wg, rg, tot, hg_o, wg_o, rg_o, router, gain, hg_v, wg_v, rg_v, tot_v, ro_v, rsem, wsem):
    parts = [(tot, tot_v, None)]
    for src, via, dst, rows in ((wg, wg_v, wg_o, 240), (hg, hg_v, hg_o, 480), (rg, rg_v, rg_o, 1440)):
        for r in range(0, src.shape[0], rows):
            at = pl.ds(r, rows)
            parts.append((src.at[at], via.at[at], dst.at[at]))
    reads = [pltpu.make_async_copy(s, v, rsem.at[n]) for n, (s, v, d) in enumerate(parts)]
    for cp in reads:
        cp.start()
    writes = []
    for n, (s, v, d) in enumerate(parts):
        reads[n].wait()
        if d is None:
            ro_v[...] = tot_v[pl.ds(0, 360)].astype(F32).reshape(D, 128)
            cp = pltpu.make_async_copy(ro_v, router, wsem.at[n])
            cp.start()
            writes.append(cp)
            rows = tot_v[pl.ds(360, 3)].astype(F32).reshape(24, 128)
            for j in range(23):
                m = min(128, D - 128 * j)
                gain[pl.ds(128 * j, m)] = rows[j : j + 1, 0:m].reshape(m)
        else:
            cp = pltpu.make_async_copy(v, d, wsem.at[n])
            cp.start()
            writes.append(cp)
    for cp in writes:
        cp.wait()


def on_device(residual, norm_gain, router_weight, out_grad, expert_ids, hidden, down_weight):
    vm = pl.BlockSpec(memory_space=pltpu.VMEM)
    hbm = pl.BlockSpec(memory_space=pl.ANY)
    dma = pltpu.SemaphoreType.DMA
    scratch = [
        pltpu.VMEM((D, 128), BF), pltpu.VMEM((D, 128), BF), pltpu.VMEM((D,), F32), pltpu.VMEM((D, 128), BF),
        pltpu.VMEM((4, 128), jnp.int32), pltpu.VMEM((D, 128), BF), pltpu.VMEM((384, 8, 128), BF),
        pltpu.VMEM((FF, 768), BF), pltpu.VMEM((FF, D), BF), pltpu.VMEM((FF, 768), F32), pltpu.VMEM((FF, 768), BF),
        pltpu.VMEM((128, 128), F32), pltpu.VMEM((128, 128), F32), pltpu.VMEM((D, 128), BF), pltpu.VMEM((D, 128), F32),
        pltpu.VMEM((128, 1, 128), F32), pltpu.VMEM((128, 1, 128), F32),
        pltpu.VMEM((384, 8, 128), BF), pltpu.VMEM((3, 3, 32, 8, 128), BF), pltpu.VMEM((3, 32, 8, 128), BF),
        pltpu.VMEM((3, 32, 8, 128), BF), pltpu.VMEM((24, 128), F32), pltpu.VMEM((768, D), BF),
        pltpu.VMEM((FF, 768), BF), pltpu.VMEM((FF, 768), BF), pltpu.VMEM((FF, 576), BF),
    ]
    scratch += [pltpu.VMEM((4, 128, 128), BF) for _ in GDIMS]
    scratch += [pltpu.VMEM((4, 128, 128), BF)]
    scratch += [pltpu.VMEM((768, 512), BF) for _ in GDIMS]
    scratch += [pltpu.VMEM((768, 128), BF) for _ in GDIMS]
    scratch += [pltpu.VMEM((768, 768), BF) for _ in range(2)]
    for i, (c0, nc, cw, a, p, q) in enumerate(PLAN):
        sizes = tuple(SZ[o] for o in OTHER[a])
        scratch += [
            pltpu.VMEM((cw, 512), BF), pltpu.VMEM(sizes + (3, 8, cw), BF),
            pltpu.VMEM((4,) + tuple(SZ[o] for o in OTHER[a] if o != p) + (3, 8, cw), BF),
            pltpu.VMEM(sizes + (3, 8, cw), BF),
        ]
    ng = len(GDIMS)
    scratch += [dma((ng, 3)), dma((ng, 3)), dma((3,)), dma((3,)), dma((NCH, 4)), dma((NCH, 4))]
    scratch += [dma((NCH, 3)), dma((NCH, 3)), dma((NCH, 7)), dma((NCH, 7))]
    scratch += [dma(()), dma(()), dma((3, 3)), dma((3, 3)), dma((3,)), dma((3,))]
    scratch += [dma((3,)), dma((3,)), dma((3, 3)), dma((3, 3)), dma((14,))]
    hidden_grad, weight_grad, residual_grad, total = pl.pallas_call(
        kernel,
        name="routed",
        out_shape=(
            jax.ShapeDtypeStruct((FF, 768), BF),
            jax.ShapeDtypeStruct((FF, D), BF),
            jax.ShapeDtypeStruct((D, 128), BF),
            jax.ShapeDtypeStruct((384, 8, 128), BF),
        ),
        in_specs=[hbm] * 7,
        out_specs=(hbm,) * 4,
        scratch_shapes=scratch,
        compiler_params=pltpu.CompilerParams(
            collective_id=0, has_side_effects=True, vmem_limit_bytes=67043328
        ),
    )(out_grad.T, residual.T, norm_gain, router_weight, expert_ids.T, hidden[0].T, down_weight[0])
    nparts = 1 + FF // 240 + FF // 480 + D // 1440
    hidden_grad, weight_grad, residual_grad, router_grad, gain_grad = pl.pallas_call(
        finish,
        name="finish",
        out_shape=(
            jax.ShapeDtypeStruct((FF, 768), BF),
            jax.ShapeDtypeStruct((FF, D), BF),
            jax.ShapeDtypeStruct((D, 128), BF),
            jax.ShapeDtypeStruct((D, 128), F32),
            jax.ShapeDtypeStruct((D,), F32),
        ),
        in_specs=[hbm, hbm, hbm, hbm],
        out_specs=(hbm, hbm, hbm, hbm, vm),
        scratch_shapes=[
            pltpu.VMEM((FF, 768), BF), pltpu.VMEM((FF, D), BF), pltpu.VMEM((D, 128), BF),
            pltpu.VMEM((384, 8, 128), BF), pltpu.VMEM((D, 128), F32), dma((nparts,)), dma((nparts,)),
        ],
        compiler_params=pltpu.CompilerParams(vmem_limit_bytes=67043328),
    )(hidden_grad, weight_grad, residual_grad, total)
    return hidden_grad.T[None], weight_grad[None], residual_grad.T, router_grad, gain_grad


def solution(mesh):
    finer = Mesh(mesh.devices.reshape(4, 4, 2, mesh.shape["dp"]), AX)
    rows = P(AX, None)
    cube = P(AX, None, None)
    return jax.shard_map(
        on_device,
        mesh=finer,
        in_specs=(rows, P(), P(), rows, rows, cube, cube),
        out_specs=(cube, cube, rows, P(), P()),
        check_vma=False,
    )
```

```python
import functools

import jax
import jax.numpy as jnp
from jax import lax
from jax.experimental import pallas as pl
from jax.experimental.pallas import tpu as pltpu
from jax.sharding import Mesh
from jax.sharding import PartitionSpec as P

AX = ("ep_0", "ep_1", "ep_2", "dp")
SZ = (4, 4, 2, 4)
Z, X, CORE, Y = 0, 1, 2, 3
STRIDE = (32, 8, 4, 1)
MESH = pl.DeviceIdType.MESH
D = 2880
FF = 1440
BF = jnp.bfloat16
F32 = jnp.float32

PLAN = (
    (0, 512, 512, Y, Z, X),
    (512, 512, 512, Z, X, Y),
    (1024, 512, 512, X, Y, Z),
    (1536, 256, 256, Y, X, Z),
    (1792, 256, 256, Z, Y, X),
    (2048, 256, 256, X, Z, Y),
    (2304, 256, 256, Y, Z, X),
    (2560, 256, 256, Z, X, Y),
    (2816, 64, 128, X, Y, Z),
)
NCH = len(PLAN)
LAST = NCH - 1
PARTS = (0, 1536, 2304, 2880)
OUT_COLS = ((0, 768), (768, 768), (1536, 768), (2304, 576))
GDIMS = tuple(dict.fromkeys(c[3] for c in PLAN))
FB = 480
NT = (((1,), (1,)), ((), ()))
TN = (((0,), (0,)), ((), ()))
COLORS = ((Z, (X, CORE, Y)), (X, (Z, CORE, Y)), (Y, (Z, X, CORE)))
OTHER = {Z: (X, CORE, Y), X: (Z, CORE, Y), Y: (Z, X, CORE)}


def plane_offsets(dims):
    out = []
    for a in range(SZ[dims[0]]):
        for b in range(SZ[dims[1]]):
            for c in range(SZ[dims[2]]):
                if (a, b, c) != (0, 0, 0):
                    t = [0, 0, 0, 0]
                    t[dims[0]], t[dims[1]], t[dims[2]] = a, b, c
                    out.append(tuple(t))
    return out


def spread(offsets):
    def hops(t):
        return sum(min(t[i], SZ[i] - t[i]) for i in (Z, X, Y))

    return sorted(offsets, key=lambda t: -hops(t))


def ring_offset(dim, d):
    t = [0, 0, 0, 0]
    t[dim] = d
    return tuple(t)


PEERS = [
    (z, x, c, y)
    for z in range(4) for x in range(4) for c in range(2) for y in range(4)
    if (z, x, c, y) != (0, 0, 0, 0)
]


def kernel(*refs):
    names = (
        ["og_h", "res_h", "gain_h", "rw_h", "ids_h", "hid_h", "w_h"]
        + ["hg_h", "wg_h", "rg_h", "tot_h"]
        + ["og", "res", "gain", "rw", "ids", "rg", "tot", "hid", "w", "acc", "hgs", "mt", "prob", "normedt", "gc"]
        + ["rsc", "rr", "xs", "ar1", "as2", "ar2", "gv", "rows", "wgs0", "wgs1", "wgs3", "idg"]
    )
    ng = len(GDIMS)
    names += [f"mg{g}" for g in range(ng)] + ["pg"] + [f"pb{g}" for g in range(ng)]
    names += [f"pick{g}" for g in range(ng)]
    names += [f"perm{a}" for a in (Z, X)]
    for i in range(NCH):
        names += [f"tok{i}", f"sel{i}", f"b1_{i}", f"fin{i}"]
    names += ["s_m", "r_m", "s_p", "r_p", "s_ag", "r_ag", "s_p1", "r_p1", "s_p2", "r_p2"]
    names += ["s_ret", "r_ret", "s_a1", "r_a1", "s_a2", "r_a2"]
    names += ["s_g2", "r_g2", "s_g1", "r_g1", "loc"]
    assert len(names) == len(refs)
    k = dict(zip(names, refs))
    me = [lax.axis_index(a) for a in AX]

    def dev(t):
        return tuple(
            lax.rem(me[i] + t[i], SZ[i]) if t[i] else me[i] for i in range(4)
        )

    def coord(dim, d):
        return lax.rem(me[dim] + d, SZ[dim]) if d else me[dim]

    def remote(src, dst, ssem, rsem, t):
        return pltpu.make_async_remote_copy(
            src_ref=src, dst_ref=dst, send_sem=ssem, recv_sem=rsem,
            device_id=dev(t), device_id_type=MESH,
        )

    pending = []

    def launch(src, dst, ssem, rsem, t):
        remote(src, dst, ssem, rsem, t).start()

    def wait_all(ref, sem):
        pltpu.make_async_copy(ref, ref, sem).wait()

    fetch = {}
    for n, name in enumerate(("ids", "gain", "og", "res", "rw")):
        fetch[name] = pltpu.make_async_copy(k[name + "_h"], k[name], k["loc"].at[7 + n])
        fetch[name].start()
    barrier = pltpu.get_barrier_semaphore()
    for t in PEERS:
        pl.semaphore_signal(barrier, inc=1, device_id=dev(t), device_id_type=MESH)
    w_copy = pltpu.make_async_copy(k["w_h"], k["w"], k["loc"].at[0])
    w_copy.start()
    hid_copy = pltpu.make_async_copy(k["hid_h"], k["hid"], k["loc"].at[1])
    hid_copy.start()

    e_row = lax.broadcasted_iota(jnp.int32, (128, 128), 0)
    t_col = lax.broadcasted_iota(jnp.int32, (128, 128), 1)
    fetch["ids"].wait()
    earlier = jnp.where(e_row < t_col, 1.0, 0.0).astype(BF)

    def marks_of(ids):
        match = e_row == ids[0:1, :]
        for j in range(1, 4):
            match = match | (e_row == ids[j : j + 1, :])
        ones = match.astype(F32)
        count = jnp.dot(ones.astype(BF), earlier, preferred_element_type=F32)
        return match, ones * (count + 1.0)

    match, mt = marks_of(k["ids"][...])
    k["mt"][...] = mt
    for g, a in enumerate(GDIMS):
        k[f"mg{g}"][me[a]] = mt.astype(BF)
    nl, cl = PLAN[LAST][1:3]
    k[f"tok{LAST}"][nl:cl, :] = jnp.zeros((cl - nl, 512), BF)

    group = lax.broadcasted_iota(jnp.int32, (32, 24, 128), 0)
    inner_row = lax.broadcasted_iota(jnp.int32, (32, 24, 128), 1)
    lane3 = lax.broadcasted_iota(jnp.int32, (32, 24, 128), 2)
    src_of = (
        jnp.where(inner_row >= 6, 1, 0) + jnp.where(inner_row >= 12, 1, 0) + jnp.where(inner_row >= 18, 1, 0)
    )
    want = (inner_row - 6 * src_of + 1).astype(F32).reshape(768, 128)
    src_flat = src_of.reshape(768, 128)
    for g, a in enumerate(GDIMS):
        o = OTHER[a]
        n1, n2 = SZ[o[1]] * SZ[o[2]], SZ[o[2]]
        expert = STRIDE[a] * me[a] + STRIDE[o[0]] * (group // n1)
        expert = expert + STRIDE[o[1]] * ((group // n2) % SZ[o[1]]) + STRIDE[o[2]] * (group % n2)
        k[f"pick{g}"][...] = jnp.where(expert == lane3, 1.0, 0.0).reshape(768, 128).astype(BF)
    eye = e_row == t_col
    fetch["gain"].wait()
    for j in range(23):
        n = min(128, D - 128 * j)
        row = k["gain"][pl.ds(128 * j, n)].reshape(1, n)
        col = jnp.sum(jnp.where(eye[:n, :n], row, 0.0), -1, keepdims=True)
        k["gc"][128 * j : 128 * j + n, :] = jnp.broadcast_to(col, (n, 128))
    fetch["og"].wait()
    pl.semaphore_wait(barrier, len(PEERS))

    for g, a in enumerate(GDIMS):
        for d in (2, 1, 3):
            launch(k["ids"], k["idg"].at[g, d - 1], k["s_m"], k["r_m"].at[g], ring_offset(a, d))
    pending.append((k["idg"], k["s_m"]))
    def lanes_of(a, d):
        return pl.ds(pl.multiple_of(coord(a, d) * 128, 128), 128)

    def gather(i):
        c0, nc, cw, a, p, q = PLAN[i]
        src = k["og"].at[pl.ds(c0, nc)]
        dst = k[f"tok{i}"].at[pl.ds(0, nc), lanes_of(a, 0)]
        for d in (1, 3):
            launch(src, dst, k["s_ag"].at[i], k["r_ag"].at[i, 0], ring_offset(a, d))

    def relay(i):
        c0, nc, cw, a, p, q = PLAN[i]
        half = nc // 2
        tok = k[f"tok{i}"]
        wait_all(tok.at[pl.ds(0, nc), pl.ds(0, 256)], k["r_ag"].at[i, 0])
        for n, d in enumerate((1, 3)):
            piece = tok.at[pl.ds(n * half, half), lanes_of(a, 4 - d)]
            launch(piece, piece, k["s_ag"].at[i], k["r_ag"].at[i, 1], ring_offset(a, d))
        pending.append((tok.at[pl.ds(0, nc), pl.ds(0, 384)], k["s_ag"].at[i]))

    for i in range(NCH):
        gather(i)
    for i, (c0, nc, cw, a, p, q) in enumerate(PLAN):
        k[f"tok{i}"][0:nc, pl.ds(pl.multiple_of(me[a] * 128, 128), 128)] = k["og"][c0 : c0 + nc, :]

    fetch["res"].wait()
    fetch["rw"].wait()
    floated = k["res"][...].astype(F32)
    inv = lax.rsqrt(jnp.mean(floated * floated, 0, keepdims=True) + 1e-05)
    normed = (floated * inv * k["gc"][...]).astype(BF)
    k["normedt"][...] = normed
    logits = lax.dot_general(k["rw"][...], normed, TN, preferred_element_type=F32)
    expo = jnp.where(match, jnp.exp(logits), 0.0)
    prob = expo / jnp.sum(expo, 0, keepdims=True)
    k["prob"][...] = prob
    pa = PLAN[LAST][3]
    k["pg"][me[pa]] = prob.astype(BF)
    own = k["pg"].at[me[pa]]
    for d in (2, 1, 3):
        launch(own, own, k["s_p"], k["r_p"], ring_offset(pa, d))
    pending.append((k["pg"].at[pl.ds(0, 3)], k["s_p"]))

    for g, a in enumerate(GDIMS):
        wait_all(k["idg"].at[g], k["r_m"].at[g])
        for d in (1, 2, 3):
            k[f"mg{g}"][coord(a, 4 - d)] = marks_of(k["idg"][g, d - 1])[1].astype(BF)

    def first_ring(i):
        c0, nc, cw, a, p, q = PLAN[i]
        g = GDIMS.index(a)
        pb = k[f"pb{g}"]
        if i < len(GDIMS):
            for s in range(4):
                marks = jnp.dot(k[f"pick{g}"][...], k[f"mg{g}"][s], preferred_element_type=F32)
                hit = (marks == want) & (src_flat == s)
                pb[:, s * 128 : (s + 1) * 128] = jnp.where(hit, 1.0, 0.0).astype(BF)
        wait_all(k[f"tok{i}"].at[pl.ds(0, nc), pl.ds(0, 128)], k["r_ag"].at[i, 1])
        rows = lax.dot_general(pb[...], k[f"tok{i}"][...], NT, preferred_element_type=F32)
        if i == LAST:
            wait_all(k["pg"].at[pl.ds(0, 3)], k["r_p"])
            sent = jnp.zeros((768, 128), F32)
            for s in range(4):
                weights = jnp.dot(k[f"pick{g}"][...], k["pg"][s], preferred_element_type=F32)
                sent = sent + pb[:, s * 128 : (s + 1) * 128].astype(F32) * weights
            sent = jnp.sum(sent, -1, keepdims=True)
            lane = lax.broadcasted_iota(jnp.int32, (768, cw), 1)
            rows = jnp.where(lane >= nc, sent, rows)
        others = OTHER[a]
        sel, b1 = k[f"sel{i}"], k[f"b1_{i}"]
        sel[...] = rows.reshape(tuple(SZ[o] for o in others) + (3, 8, cw)).astype(BF)
        for d in (2, 1, 3):
            spot = tuple(coord(p, d) if o == p else slice(None) for o in others)
            launch(sel.at[spot], b1.at[me[p]], k["s_p1"].at[i], k["r_p1"].at[i], ring_offset(p, d))
        pending.append((b1.at[pl.ds(0, 3)], k["s_p1"].at[i]))
        b1[me[p]] = sel[tuple(me[p] if o == p else slice(None) for o in others)]

    for i in range(6):
        relay(i)
    for i in (0, 1, 2):
        first_ring(i)
    for i in (6, 7, 8):
        relay(i)
    for i in (3, 4, 5):
        first_ring(i)

    slot = lax.broadcasted_iota(jnp.int32, (768, 128), 0)
    lane = lax.broadcasted_iota(jnp.int32, (768, 128), 1)
    src = (slot * 10923) // 65536
    rest = slot - 6 * src
    from_z = (src % 32) * 24 + (src // 32) * 6 + rest
    from_x = ((src // 32) * 8 + src % 8) * 24 + ((src // 8) % 4) * 6 + rest
    for a, origin in ((Z, from_z), (X, from_x)):
        for j in range(6):
            k[f"perm{a}"][:, 128 * j : 128 * j + 128] = jnp.where(origin == lane + 128 * j, 1.0, 0.0).astype(BF)
    w_copy.wait()
    hid_copy.wait()

    def second_ring(i):
        c0, nc, cw, a, p, q = PLAN[i]
        wait_all(k[f"b1_{i}"].at[pl.ds(0, 3)], k["r_p1"].at[i])
        others = OTHER[a]
        left = tuple(o for o in others if o != p)
        spot = tuple(slice(None) if o == p else me[o] for o in others)
        b1, fin = k[f"b1_{i}"], k[f"fin{i}"]

        def part_of(dq, dc):
            return (slice(None),) + tuple(coord(q, dq) if o == q else coord(CORE, dc) for o in left)

        for dq in (2, 1, 3, 0):
            for dc in (0, 1):
                if dq == 0 and dc == 0:
                    continue
                t = [0, 0, 0, 0]
                t[q], t[CORE] = dq, dc
                launch(b1.at[part_of(dq, dc)], fin.at[spot], k["s_p2"].at[i], k["r_p2"].at[i], tuple(t))
        pending.append((k["rows"].at[pl.ds(0, 672), pl.ds(0, cw)], k["s_p2"].at[i]))
        fin[spot] = b1[part_of(0, 0)]

    def arrived(i):
        c0, nc, cw, a, p, q = PLAN[i]
        wait_all(k["rows"].at[pl.ds(0, 672), pl.ds(0, cw)], k["r_p2"].at[i])
        rows = k[f"fin{i}"][...].reshape(96, 8, cw).astype(F32).reshape(768, cw)
        if a != Y:
            rows = jnp.dot(k[f"perm{a}"][...], rows.astype(BF), preferred_element_type=F32)
        weight = None
        if i == LAST:
            spot = lax.broadcasted_iota(jnp.int32, (16, cw), 1)
            weight = rows[:, nc : nc + 1], lax.dot_general(
                jnp.where(spot == nc, 1.0, 0.0).astype(BF), rows.astype(BF), NT, preferred_element_type=F32
            )[0:1]
            rows = rows[:, :nc]
        k["rows"][:, c0 : c0 + nc] = rows.astype(BF)
        return weight

    def inner_part(h, first=0, last=FF // FB):
        cols = slice(PARTS[h], PARTS[h + 1])

        def step(n, carry):
            at = pl.ds(pl.multiple_of(n * FB, FB), FB)
            part = lax.dot_general(k["w"][at, cols], k["rows"][:, cols], NT, preferred_element_type=F32)
            if h == 0:
                k["acc"][at, :] = part
            else:
                k["acc"][at, :] += part
            return carry

        lax.fori_loop(first, last, step, 0)

    for i in (0, 1, 2):
        second_ring(i)
    for i in (6, 7, 8):
        first_ring(i)
    for i in (3, 4, 5):
        second_ring(i)
    for i in (0, 1, 2):
        arrived(i)
    inner_part(0, 0, 2)
    for i in (6, 7, 8):
        second_ring(i)
    inner_part(0, 2, 3)
    for i in (3, 4, 5):
        arrived(i)
    inner_part(1)
    for i in (6, 7, 8):
        weight = arrived(i)
    weight_col, weight_row = weight
    inner_part(2)

    out_cps = {}

    def weight_grad(i):
        c0, nc = OUT_COLS[i]
        scaled = (weight_col * k["rows"][:, c0 : c0 + nc].astype(F32)).astype(BF)
        out = k[("wgs0", "wgs1", "wgs0", "wgs3")[i]]
        if i == 2:
            out_cps[0].wait()

        def step(n, carry):
            at = pl.ds(pl.multiple_of(n * FB, FB), FB)
            out[at, :] = jnp.dot(k["hid"][at, :], scaled, preferred_element_type=F32).astype(BF)
            return carry

        lax.fori_loop(0, FF // FB, step, 0)
        cp = pltpu.make_async_copy(out, k["wg_h"].at[:, pl.ds(c0, nc)], k["loc"].at[2 + i])
        cp.start()
        out_cps[i] = cp

    slot_score = jnp.sum(k["acc"][...] * k["hid"][...].astype(F32), 0, keepdims=True)
    hi = slot_score.astype(BF)
    lo = (slot_score - hi.astype(F32)).astype(BF)
    g_row = lax.broadcasted_iota(jnp.int32, (128, 768), 0)
    g_lane = lax.broadcasted_iota(jnp.int32, (128, 768), 1)
    inside = (g_lane >= g_row * 6) & (g_lane < g_row * 6 + 6)
    place = jnp.where(rest == lane, 1.0, 0.0).astype(BF)
    packed = jnp.zeros((128, 128), F32)
    for part in (hi, lo):
        spread_out = jnp.where(inside, part.astype(F32), 0.0).astype(BF)
        packed = packed + jnp.dot(spread_out, place, preferred_element_type=F32)
    k["rsc"][...] = packed.reshape(128, 1, 128)
    mine = sum(me[o] * STRIDE[o] for o in range(4))
    for t in spread(PEERS):
        there = sum(coord(o, t[o]) * STRIDE[o] for o in range(4))
        remote(k["rsc"].at[there], k["rr"].at[mine], k["s_ret"], k["r_ret"], t).start()
    k["rr"][mine] = k["rsc"][mine]
    k["hgs"][...] = (weight_row * k["acc"][...]).astype(BF)
    cp = pltpu.make_async_copy(k["hgs"], k["hg_h"], k["loc"].at[6])
    cp.start()
    out_cps[4] = cp
    weight_grad(0)
    few = k["rsc"].at[pl.ds(0, 127)]
    pltpu.make_async_copy(few, few, k["r_ret"]).wait()

    back = k["rr"][...].reshape(128, 128)
    mt = k["mt"][...]
    prob = k["prob"][...]
    score = jnp.zeros((128, 128), F32)
    for r in range(6):
        score = score + jnp.where(mt == float(r + 1), back[:, r : r + 1], 0.0)
    grad_t = prob * (score - jnp.sum(prob * score, 0, keepdims=True))
    grad = grad_t.T

    def halves(v):
        top = v.astype(BF)
        return top, (v - top.astype(F32)).astype(BF)

    hi, lo = halves(grad)
    xs = k["xs"]
    def router_rows(n):
        at = slice(1024 * n, min(D, 1024 * n + 1024))
        local = jnp.dot(k["normedt"][at, :], hi, preferred_element_type=F32) + jnp.dot(
            k["normedt"][at, :], lo, preferred_element_type=F32
        )
        blocks = (at.stop - at.start) // 8
        xs[pl.ds(128 * n, blocks)] = local.reshape(blocks, 8, 128).astype(BF)

    def send_color(n):
        a = COLORS[n][0]
        for d in (2, 1, 3):
            piece = xs.at[pl.ds(pl.multiple_of(128 * n + 32 * coord(a, d), 32), 32)]
            launch(piece, k["ar1"].at[n, d - 1], k["s_a1"].at[n], k["r_a1"].at[n], ring_offset(a, d))
        pending.append((k["ar1"].at[n], k["s_a1"].at[n]))

    for n in range(2):
        router_rows(n)
        send_color(n)
    router_rows(2)
    hi, lo = halves(grad_t)
    normed_grad = jnp.dot(k["rw"][...], hi, preferred_element_type=F32) + jnp.dot(
        k["rw"][...], lo, preferred_element_type=F32
    )
    floated = k["res"][...].astype(F32)
    inv = lax.rsqrt(jnp.mean(floated * floated, 0, keepdims=True) + 1e-05)
    unit = floated * inv
    gain_col = jnp.sum(normed_grad * unit, -1, keepdims=True)
    k["gv"][...] = jnp.zeros_like(k["gv"])
    for j in range(23):
        n = min(128, D - 128 * j)
        col = gain_col[128 * j : 128 * j + n]
        k["gv"][j : j + 1, 0:n] = jnp.sum(jnp.where(eye[:n, :n], col, 0.0), 0, keepdims=True)
    xs[pl.ds(360, 3)] = k["gv"][...].reshape(3, 8, 128).astype(BF)
    xs[pl.ds(363, 21)] = jnp.zeros((21, 8, 128), BF)
    send_color(2)
    upper = normed_grad * k["gc"][...]
    k["rg"][...] = (inv * (upper - unit * jnp.mean(upper * unit, 0, keepdims=True))).astype(BF)
    cp = pltpu.make_async_copy(k["rg"], k["rg_h"], k["loc"].at[12])
    cp.start()
    out_cps[5] = cp
    weight_grad(1)

    for n, (a, others) in enumerate(COLORS):
        wait_all(k["ar1"].at[n], k["r_a1"].at[n])
        total = xs[pl.ds(pl.multiple_of(128 * n + 32 * me[a], 32), 32)].astype(F32)
        for d in range(3):
            total = total + k["ar1"][n, d].astype(F32)
        k["as2"][n] = total.astype(BF)
        ring = (SZ[others[1]] * SZ[others[2]], SZ[others[2]], 1)

        def rank(t):
            return sum(coord(o, t[o]) * s for o, s in zip(others, ring))

        here = rank((0, 0, 0, 0))
        for t in spread(plane_offsets(others)):
            cp = remote(k["as2"].at[n, rank(t)], k["ar2"].at[n, here], k["s_a2"].at[n], k["r_a2"].at[n], t)
            cp.start()
        k["ar2"][n, here] = k["as2"][n, here]
    weight_grad(2)
    tot = k["tot"]
    for n, (a, others) in enumerate(COLORS):
        few = k["as2"].at[n, pl.ds(0, 31)]
        pltpu.make_async_copy(few, few, k["r_a2"].at[n]).wait()
        ring = (SZ[others[1]] * SZ[others[2]], SZ[others[2]], 1)
        here = sum(me[o] * s for o, s in zip(others, ring))
        done = jnp.sum(k["ar2"][n].astype(F32), 0)
        at = 128 * n + 32 * me[a] + here
        tot[at] = done.astype(BF)
        for t in spread(plane_offsets(others)):
            cp = remote(tot.at[at], tot.at[at], k["s_g2"].at[n], k["r_g2"].at[n], t)
            cp.start()
    weight_grad(3)
    for n, (a, others) in enumerate(COLORS):
        few = k["as2"].at[n, pl.ds(0, 31)]
        pltpu.make_async_copy(few, few, k["r_g2"].at[n]).wait()
        piece = tot.at[pl.ds(pl.multiple_of(128 * n + 32 * me[a], 32), 32)]
        for d in (2, 1, 3):
            launch(piece, piece, k["s_g1"].at[n], k["r_g1"].at[n], ring_offset(a, d))
        pending.append((tot.at[pl.ds(0, 96)], k["s_g1"].at[n]))
    for n in range(3):
        wait_all(tot.at[pl.ds(0, 96)], k["r_g1"].at[n])
        blocks = pl.ds(128 * n, 128)
        cp = pltpu.make_async_copy(k["tot"].at[blocks], k["tot_h"].at[blocks], k["loc"].at[13 + n])
        cp.start()
        out_cps[6 + n] = cp
    for ref, sem in pending:
        wait_all(ref, sem)
    few = k["rsc"].at[pl.ds(0, 127)]
    pltpu.make_async_copy(few, few, k["s_ret"]).wait()
    for n in range(3):
        few = k["as2"].at[n, pl.ds(0, 31)]
        pltpu.make_async_copy(few, few, k["s_a2"].at[n]).wait()
        pltpu.make_async_copy(few, few, k["s_g2"].at[n]).wait()
    for i, cp in out_cps.items():
        if i != 0:
            cp.wait()


def finish(hg, wg, rg, tot, hg_o, wg_o, rg_o, router, gain, hg_v, wg_v, rg_v, tot_v, ro_v, rsem, wsem):
    parts = [(tot, tot_v, None)]
    for src, via, dst, rows in ((wg, wg_v, wg_o, 240), (hg, hg_v, hg_o, 480), (rg, rg_v, rg_o, 1440)):
        for r in range(0, src.shape[0], rows):
            at = pl.ds(r, rows)
            parts.append((src.at[at], via.at[at], dst.at[at]))
    reads = [pltpu.make_async_copy(s, v, rsem.at[n]) for n, (s, v, d) in enumerate(parts)]
    for cp in reads:
        cp.start()
    writes = []
    for n, (s, v, d) in enumerate(parts):
        reads[n].wait()
        if d is None:
            ro_v[...] = tot_v[pl.ds(0, 360)].astype(F32).reshape(D, 128)
            cp = pltpu.make_async_copy(ro_v, router, wsem.at[n])
            cp.start()
            writes.append(cp)
            rows = tot_v[pl.ds(360, 3)].astype(F32).reshape(24, 128)
            for j in range(23):
                m = min(128, D - 128 * j)
                gain[pl.ds(128 * j, m)] = rows[j : j + 1, 0:m].reshape(m)
        else:
            cp = pltpu.make_async_copy(v, d, wsem.at[n])
            cp.start()
            writes.append(cp)
    for cp in writes:
        cp.wait()


def on_device(residual, norm_gain, router_weight, out_grad, expert_ids, hidden, down_weight):
    vm = pl.BlockSpec(memory_space=pltpu.VMEM)
    hbm = pl.BlockSpec(memory_space=pl.ANY)
    dma = pltpu.SemaphoreType.DMA
    scratch = [
        pltpu.VMEM((D, 128), BF), pltpu.VMEM((D, 128), BF), pltpu.VMEM((D,), F32), pltpu.VMEM((D, 128), BF),
        pltpu.VMEM((4, 128), jnp.int32), pltpu.VMEM((D, 128), BF), pltpu.VMEM((384, 8, 128), BF),
        pltpu.VMEM((FF, 768), BF), pltpu.VMEM((FF, D), BF), pltpu.VMEM((FF, 768), F32), pltpu.VMEM((FF, 768), BF),
        pltpu.VMEM((128, 128), F32), pltpu.VMEM((128, 128), F32), pltpu.VMEM((D, 128), BF), pltpu.VMEM((D, 128), F32),
        pltpu.VMEM((128, 1, 128), F32), pltpu.VMEM((128, 1, 128), F32),
        pltpu.VMEM((384, 8, 128), BF), pltpu.VMEM((3, 3, 32, 8, 128), BF), pltpu.VMEM((3, 32, 8, 128), BF),
        pltpu.VMEM((3, 32, 8, 128), BF), pltpu.VMEM((24, 128), F32), pltpu.VMEM((768, D), BF),
        pltpu.VMEM((FF, 768), BF), pltpu.VMEM((FF, 768), BF), pltpu.VMEM((FF, 576), BF),
        pltpu.VMEM((3, 3, 4, 128), jnp.int32),
    ]
    scratch += [pltpu.VMEM((4, 128, 128), BF) for _ in GDIMS]
    scratch += [pltpu.VMEM((4, 128, 128), BF)]
    scratch += [pltpu.VMEM((768, 512), BF) for _ in GDIMS]
    scratch += [pltpu.VMEM((768, 128), BF) for _ in GDIMS]
    scratch += [pltpu.VMEM((768, 768), BF) for _ in range(2)]
    for i, (c0, nc, cw, a, p, q) in enumerate(PLAN):
        sizes = tuple(SZ[o] for o in OTHER[a])
        scratch += [
            pltpu.VMEM((cw, 512), BF), pltpu.VMEM(sizes + (3, 8, cw), BF),
            pltpu.VMEM((4,) + tuple(SZ[o] for o in OTHER[a] if o != p) + (3, 8, cw), BF),
            pltpu.VMEM(sizes + (3, 8, cw), BF),
        ]
    scratch += [dma(()), dma((3,)), dma(()), dma(()), dma((NCH,)), dma((NCH, 2))]
    scratch += [dma((NCH,)), dma((NCH,)), dma((NCH,)), dma((NCH,))]
    scratch += [dma(()), dma(()), dma((3,)), dma((3,)), dma((3,)), dma((3,))]
    scratch += [dma((3,)), dma((3,)), dma((3,)), dma((3,)), dma((16,))]
    hidden_grad, weight_grad, residual_grad, total = pl.pallas_call(
        kernel,
        name="routed",
        out_shape=(
            jax.ShapeDtypeStruct((FF, 768), BF),
            jax.ShapeDtypeStruct((FF, D), BF),
            jax.ShapeDtypeStruct((D, 128), BF),
            jax.ShapeDtypeStruct((384, 8, 128), BF),
        ),
        in_specs=[hbm] * 7,
        out_specs=(hbm,) * 4,
        scratch_shapes=scratch,
        compiler_params=pltpu.CompilerParams(
            collective_id=0, has_side_effects=True, vmem_limit_bytes=67043328
        ),
    )(out_grad.T, residual.T, norm_gain, router_weight, expert_ids.T, hidden[0].T, down_weight[0])
    nparts = 1 + FF // 240 + FF // 480 + D // 1440
    hidden_grad, weight_grad, residual_grad, router_grad, gain_grad = pl.pallas_call(
        finish,
        name="finish",
        out_shape=(
            jax.ShapeDtypeStruct((FF, 768), BF),
            jax.ShapeDtypeStruct((FF, D), BF),
            jax.ShapeDtypeStruct((D, 128), BF),
            jax.ShapeDtypeStruct((D, 128), F32),
            jax.ShapeDtypeStruct((D,), F32),
        ),
        in_specs=[hbm, hbm, hbm, hbm],
        out_specs=(hbm, hbm, hbm, hbm, vm),
        scratch_shapes=[
            pltpu.VMEM((FF, 768), BF), pltpu.VMEM((FF, D), BF), pltpu.VMEM((D, 128), BF),
            pltpu.VMEM((384, 8, 128), BF), pltpu.VMEM((D, 128), F32), dma((nparts,)), dma((nparts,)),
        ],
        compiler_params=pltpu.CompilerParams(vmem_limit_bytes=67043328),
    )(hidden_grad, weight_grad, residual_grad, total)
    return hidden_grad.T[None], weight_grad[None], residual_grad.T, router_grad, gain_grad


def solution(mesh):
    finer = Mesh(mesh.devices.reshape(4, 4, 2, mesh.shape["dp"]), AX)
    rows = P(AX, None)
    cube = P(AX, None, None)
    return jax.shard_map(
        on_device,
        mesh=finer,
        in_specs=(rows, P(), P(), rows, rows, cube, cube),
        out_specs=(cube, cube, rows, P(), P()),
        check_vma=False,
    )
```

```python
import functools

import jax
import jax.numpy as jnp
from jax import lax
from jax.experimental import pallas as pl
from jax.experimental.pallas import tpu as pltpu
from jax.sharding import Mesh
from jax.sharding import PartitionSpec as P

AX = ("ep_0", "ep_1", "ep_2", "dp")
SZ = (4, 4, 2, 4)
Z, X, CORE, Y = 0, 1, 2, 3
STRIDE = (32, 8, 4, 1)
MESH = pl.DeviceIdType.MESH
D = 2880
FF = 1440
BF = jnp.bfloat16
F32 = jnp.float32

PLAN = (
    (0, 512, 512, Y, Z, X),
    (512, 512, 512, Z, X, Y),
    (1024, 512, 512, X, Y, Z),
    (1536, 256, 256, Y, X, Z),
    (1792, 256, 256, Z, Y, X),
    (2048, 256, 256, X, Z, Y),
    (2304, 256, 256, Y, Z, X),
    (2560, 256, 256, Z, X, Y),
    (2816, 64, 128, X, Y, Z),
)
NCH = len(PLAN)
LAST = NCH - 1
PARTS = (0, 1536, 2304, 2880)
OUT_COLS = ((0, 768), (768, 768), (1536, 768), (2304, 576))
GDIMS = tuple(dict.fromkeys(c[3] for c in PLAN))
FB = 480
NT = (((1,), (1,)), ((), ()))
TN = (((0,), (0,)), ((), ()))
COLORS = ((Z, (X, CORE, Y)), (X, (Z, CORE, Y)), (Y, (Z, X, CORE)))
OTHER = {Z: (X, CORE, Y), X: (Z, CORE, Y), Y: (Z, X, CORE)}


def plane_offsets(dims):
    out = []
    for a in range(SZ[dims[0]]):
        for b in range(SZ[dims[1]]):
            for c in range(SZ[dims[2]]):
                if (a, b, c) != (0, 0, 0):
                    t = [0, 0, 0, 0]
                    t[dims[0]], t[dims[1]], t[dims[2]] = a, b, c
                    out.append(tuple(t))
    return out


def spread(offsets):
    def hops(t):
        return sum(min(t[i], SZ[i] - t[i]) for i in (Z, X, Y))

    return sorted(offsets, key=lambda t: -hops(t))


def ring_offset(dim, d):
    t = [0, 0, 0, 0]
    t[dim] = d
    return tuple(t)


PEERS = [
    (z, x, c, y)
    for z in range(4) for x in range(4) for c in range(2) for y in range(4)
    if (z, x, c, y) != (0, 0, 0, 0)
]


def kernel(*refs):
    names = (
        ["og_h", "res_h", "gain_h", "rw_h", "ids_h", "hid_h", "w_h"]
        + ["hg_h", "wg_h", "rg_h", "tot_h"]
        + ["og", "res", "gain", "rw", "ids", "rg", "tot", "hid", "w", "acc", "hgs", "mt", "prob", "normedt", "gc"]
        + ["rsc", "rr", "xs", "ar1", "as2", "ar2", "gv", "rows", "wgs0", "wgs1", "wgs3", "idg"]
    )
    ng = len(GDIMS)
    names += [f"mg{g}" for g in range(ng)] + ["pg"] + [f"pb{g}" for g in range(ng)]
    names += [f"pick{g}" for g in range(ng)]
    names += [f"perm{a}" for a in (Z, X)]
    for i in range(NCH):
        names += [f"tok{i}", f"sel{i}", f"b1_{i}", f"fin{i}"]
    names += ["s_m", "r_m", "s_p", "r_p", "s_ag", "r_ag", "s_p1", "r_p1", "s_p2", "r_p2"]
    names += ["s_ret", "r_ret", "s_a1", "r_a1", "s_a2", "r_a2"]
    names += ["s_g2", "r_g2", "s_g1", "r_g1", "loc"]
    assert len(names) == len(refs)
    k = dict(zip(names, refs))
    me = [lax.axis_index(a) for a in AX]

    def dev(t):
        return tuple(
            lax.rem(me[i] + t[i], SZ[i]) if t[i] else me[i] for i in range(4)
        )

    def coord(dim, d):
        return lax.rem(me[dim] + d, SZ[dim]) if d else me[dim]

    def remote(src, dst, ssem, rsem, t):
        return pltpu.make_async_remote_copy(
            src_ref=src, dst_ref=dst, send_sem=ssem, recv_sem=rsem,
            device_id=dev(t), device_id_type=MESH,
        )

    pending = []

    def launch(src, dst, ssem, rsem, t):
        remote(src, dst, ssem, rsem, t).start()

    def wait_all(ref, sem):
        pltpu.make_async_copy(ref, ref, sem).wait()

    fetch = {}
    for n, name in enumerate(("ids", "gain", "og", "res", "rw")):
        fetch[name] = pltpu.make_async_copy(k[name + "_h"], k[name], k["loc"].at[7 + n])
        fetch[name].start()
    barrier = pltpu.get_barrier_semaphore()
    for t in PEERS:
        pl.semaphore_signal(barrier, inc=1, device_id=dev(t), device_id_type=MESH)
    w_copy = pltpu.make_async_copy(k["w_h"], k["w"], k["loc"].at[0])
    w_copy.start()
    hid_copy = pltpu.make_async_copy(k["hid_h"], k["hid"], k["loc"].at[1])
    hid_copy.start()

    e_row = lax.broadcasted_iota(jnp.int32, (128, 128), 0)
    t_col = lax.broadcasted_iota(jnp.int32, (128, 128), 1)
    fetch["ids"].wait()
    earlier = jnp.where(e_row < t_col, 1.0, 0.0).astype(BF)

    def marks_of(ids):
        match = e_row == ids[0:1, :]
        for j in range(1, 4):
            match = match | (e_row == ids[j : j + 1, :])
        ones = match.astype(F32)
        count = jnp.dot(ones.astype(BF), earlier, preferred_element_type=F32)
        return match, ones * (count + 1.0)

    match, mt = marks_of(k["ids"][...])
    k["mt"][...] = mt
    for g, a in enumerate(GDIMS):
        k[f"mg{g}"][me[a]] = mt.astype(BF)
    nl, cl = PLAN[LAST][1:3]
    k[f"tok{LAST}"][nl:cl, :] = jnp.zeros((cl - nl, 512), BF)

    group = lax.broadcasted_iota(jnp.int32, (32, 24, 128), 0)
    inner_row = lax.broadcasted_iota(jnp.int32, (32, 24, 128), 1)
    lane3 = lax.broadcasted_iota(jnp.int32, (32, 24, 128), 2)
    src_of = (
        jnp.where(inner_row >= 6, 1, 0) + jnp.where(inner_row >= 12, 1, 0) + jnp.where(inner_row >= 18, 1, 0)
    )
    want = (inner_row - 6 * src_of + 1).astype(F32).reshape(768, 128)
    src_flat = src_of.reshape(768, 128)
    for g, a in enumerate(GDIMS):
        o = OTHER[a]
        n1, n2 = SZ[o[1]] * SZ[o[2]], SZ[o[2]]
        expert = STRIDE[a] * me[a] + STRIDE[o[0]] * (group // n1)
        expert = expert + STRIDE[o[1]] * ((group // n2) % SZ[o[1]]) + STRIDE[o[2]] * (group % n2)
        k[f"pick{g}"][...] = jnp.where(expert == lane3, 1.0, 0.0).reshape(768, 128).astype(BF)
    eye = e_row == t_col
    fetch["gain"].wait()
    for j in range(23):
        n = min(128, D - 128 * j)
        row = k["gain"][pl.ds(128 * j, n)].reshape(1, n)
        col = jnp.sum(jnp.where(eye[:n, :n], row, 0.0), -1, keepdims=True)
        k["gc"][128 * j : 128 * j + n, :] = jnp.broadcast_to(col, (n, 128))
    fetch["og"].wait()
    pl.semaphore_wait(barrier, len(PEERS))

    for g, a in enumerate(GDIMS):
        for d in (2, 1, 3):
            launch(k["ids"], k["idg"].at[g, d - 1], k["s_m"], k["r_m"].at[g], ring_offset(a, d))
    pending.append((k["idg"], k["s_m"]))
    def lanes_of(a, d):
        return pl.ds(pl.multiple_of(coord(a, d) * 128, 128), 128)

    def gather(i):
        c0, nc, cw, a, p, q = PLAN[i]
        src = k["og"].at[pl.ds(c0, nc)]
        dst = k[f"tok{i}"].at[pl.ds(0, nc), lanes_of(a, 0)]
        for d in (1, 3):
            launch(src, dst, k["s_ag"].at[i], k["r_ag"].at[i, 0], ring_offset(a, d))

    def relay(i):
        c0, nc, cw, a, p, q = PLAN[i]
        half = nc // 2
        tok = k[f"tok{i}"]
        wait_all(tok.at[pl.ds(0, nc), pl.ds(0, 256)], k["r_ag"].at[i, 0])
        for n, d in enumerate((1, 3)):
            piece = tok.at[pl.ds(n * half, half), lanes_of(a, 4 - d)]
            launch(piece, piece, k["s_ag"].at[i], k["r_ag"].at[i, 1], ring_offset(a, d))
        pending.append((tok.at[pl.ds(0, nc), pl.ds(0, 384)], k["s_ag"].at[i]))

    for i in range(NCH):
        gather(i)
    for i, (c0, nc, cw, a, p, q) in enumerate(PLAN):
        k[f"tok{i}"][0:nc, pl.ds(pl.multiple_of(me[a] * 128, 128), 128)] = k["og"][c0 : c0 + nc, :]

    fetch["res"].wait()
    fetch["rw"].wait()
    floated = k["res"][...].astype(F32)
    inv = lax.rsqrt(jnp.mean(floated * floated, 0, keepdims=True) + 1e-05)
    normed = (floated * inv * k["gc"][...]).astype(BF)
    k["normedt"][...] = normed
    logits = lax.dot_general(k["rw"][...], normed, TN, preferred_element_type=F32)
    expo = jnp.where(match, jnp.exp(logits), 0.0)
    prob = expo / jnp.sum(expo, 0, keepdims=True)
    k["prob"][...] = prob
    pa = PLAN[LAST][3]
    k["pg"][me[pa]] = prob.astype(BF)
    own = k["pg"].at[me[pa]]
    for d in (2, 1, 3):
        launch(own, own, k["s_p"], k["r_p"], ring_offset(pa, d))
    pending.append((k["pg"].at[pl.ds(0, 3)], k["s_p"]))

    for g, a in enumerate(GDIMS):
        wait_all(k["idg"].at[g], k["r_m"].at[g])
        for d in (1, 2, 3):
            k[f"mg{g}"][coord(a, 4 - d)] = marks_of(k["idg"][g, d - 1])[1].astype(BF)

    def first_ring(i):
        c0, nc, cw, a, p, q = PLAN[i]
        g = GDIMS.index(a)
        pb = k[f"pb{g}"]
        wait_all(k[f"tok{i}"].at[pl.ds(0, nc), pl.ds(0, 128)], k["r_ag"].at[i, 1])
        rows = lax.dot_general(pb[...], k[f"tok{i}"][...], NT, preferred_element_type=F32)
        if i == LAST:
            wait_all(k["pg"].at[pl.ds(0, 3)], k["r_p"])
            sent = jnp.zeros((768, 128), F32)
            for s in range(4):
                weights = jnp.dot(k[f"pick{g}"][...], k["pg"][s], preferred_element_type=F32)
                sent = sent + pb[:, s * 128 : (s + 1) * 128].astype(F32) * weights
            sent = jnp.sum(sent, -1, keepdims=True)
            lane = lax.broadcasted_iota(jnp.int32, (768, cw), 1)
            rows = jnp.where(lane >= nc, sent, rows)
        others = OTHER[a]
        sel, b1 = k[f"sel{i}"], k[f"b1_{i}"]
        sel[...] = rows.reshape(tuple(SZ[o] for o in others) + (3, 8, cw)).astype(BF)
        for d in (2, 1, 3):
            spot = tuple(coord(p, d) if o == p else slice(None) for o in others)
            launch(sel.at[spot], b1.at[me[p]], k["s_p1"].at[i], k["r_p1"].at[i], ring_offset(p, d))
        pending.append((b1.at[pl.ds(0, 3)], k["s_p1"].at[i]))
        b1[me[p]] = sel[tuple(me[p] if o == p else slice(None) for o in others)]

    for i in range(3):
        relay(i)
    for g in range(len(GDIMS)):
        for s in range(4):
            marks = jnp.dot(k[f"pick{g}"][...], k[f"mg{g}"][s], preferred_element_type=F32)
            hit = (marks == want) & (src_flat == s)
            k[f"pb{g}"][:, s * 128 : (s + 1) * 128] = jnp.where(hit, 1.0, 0.0).astype(BF)
    for i in range(3, 6):
        relay(i)
    for i in (0, 1, 2):
        first_ring(i)
    for i in (6, 7, 8):
        relay(i)
    for i in (3, 4, 5):
        first_ring(i)

    slot = lax.broadcasted_iota(jnp.int32, (768, 128), 0)
    lane = lax.broadcasted_iota(jnp.int32, (768, 128), 1)
    src = (slot * 10923) // 65536
    rest = slot - 6 * src
    from_z = (src % 32) * 24 + (src // 32) * 6 + rest
    from_x = ((src // 32) * 8 + src % 8) * 24 + ((src // 8) % 4) * 6 + rest
    for a, origin in ((Z, from_z), (X, from_x)):
        for j in range(6):
            k[f"perm{a}"][:, 128 * j : 128 * j + 128] = jnp.where(origin == lane + 128 * j, 1.0, 0.0).astype(BF)
    w_copy.wait()
    hid_copy.wait()

    def second_ring(i):
        c0, nc, cw, a, p, q = PLAN[i]
        wait_all(k[f"b1_{i}"].at[pl.ds(0, 3)], k["r_p1"].at[i])
        others = OTHER[a]
        left = tuple(o for o in others if o != p)
        spot = tuple(slice(None) if o == p else me[o] for o in others)
        b1, fin = k[f"b1_{i}"], k[f"fin{i}"]

        def part_of(dq, dc):
            return (slice(None),) + tuple(coord(q, dq) if o == q else coord(CORE, dc) for o in left)

        for dq in (2, 1, 3, 0):
            for dc in (0, 1):
                if dq == 0 and dc == 0:
                    continue
                t = [0, 0, 0, 0]
                t[q], t[CORE] = dq, dc
                launch(b1.at[part_of(dq, dc)], fin.at[spot], k["s_p2"].at[i], k["r_p2"].at[i], tuple(t))
        pending.append((k["rows"].at[pl.ds(0, 672), pl.ds(0, cw)], k["s_p2"].at[i]))
        fin[spot] = b1[part_of(0, 0)]

    def arrived(i):
        c0, nc, cw, a, p, q = PLAN[i]
        wait_all(k["rows"].at[pl.ds(0, 672), pl.ds(0, cw)], k["r_p2"].at[i])
        rows = k[f"fin{i}"][...].reshape(96, 8, cw).astype(F32).reshape(768, cw)
        if a != Y:
            rows = jnp.dot(k[f"perm{a}"][...], rows.astype(BF), preferred_element_type=F32)
        weight = None
        if i == LAST:
            spot = lax.broadcasted_iota(jnp.int32, (16, cw), 1)
            weight = rows[:, nc : nc + 1], lax.dot_general(
                jnp.where(spot == nc, 1.0, 0.0).astype(BF), rows.astype(BF), NT, preferred_element_type=F32
            )[0:1]
            rows = rows[:, :nc]
        k["rows"][:, c0 : c0 + nc] = rows.astype(BF)
        return weight

    def inner_part(h, first=0, last=FF // FB):
        cols = slice(PARTS[h], PARTS[h + 1])

        def step(n, carry):
            at = pl.ds(pl.multiple_of(n * FB, FB), FB)
            part = lax.dot_general(k["w"][at, cols], k["rows"][:, cols], NT, preferred_element_type=F32)
            if h == 0:
                k["acc"][at, :] = part
            else:
                k["acc"][at, :] += part
            return carry

        lax.fori_loop(first, last, step, 0)

    for i in (0, 1, 2):
        second_ring(i)
    for i in (6, 7, 8):
        first_ring(i)
    for i in (3, 4, 5):
        second_ring(i)
    for i in (0, 1, 2):
        arrived(i)
    inner_part(0, 0, 2)
    for i in (6, 7, 8):
        second_ring(i)
    inner_part(0, 2, 3)
    for i in (3, 4, 5):
        arrived(i)
    inner_part(1)
    for i in (6, 7, 8):
        weight = arrived(i)
    weight_col, weight_row = weight
    inner_part(2)

    out_cps = {}

    def weight_grad(i):
        c0, nc = OUT_COLS[i]
        scaled = (weight_col * k["rows"][:, c0 : c0 + nc].astype(F32)).astype(BF)
        out = k[("wgs0", "wgs1", "wgs0", "wgs3")[i]]
        if i == 2:
            out_cps[0].wait()

        def step(n, carry):
            at = pl.ds(pl.multiple_of(n * FB, FB), FB)
            out[at, :] = jnp.dot(k["hid"][at, :], scaled, preferred_element_type=F32).astype(BF)
            return carry

        lax.fori_loop(0, FF // FB, step, 0)
        cp = pltpu.make_async_copy(out, k["wg_h"].at[:, pl.ds(c0, nc)], k["loc"].at[2 + i])
        cp.start()
        out_cps[i] = cp

    slot_score = jnp.sum(k["acc"][...] * k["hid"][...].astype(F32), 0, keepdims=True)
    hi = slot_score.astype(BF)
    lo = (slot_score - hi.astype(F32)).astype(BF)
    g_row = lax.broadcasted_iota(jnp.int32, (128, 768), 0)
    g_lane = lax.broadcasted_iota(jnp.int32, (128, 768), 1)
    inside = (g_lane >= g_row * 6) & (g_lane < g_row * 6 + 6)
    place = jnp.where(rest == lane, 1.0, 0.0).astype(BF)
    packed = jnp.zeros((128, 128), F32)
    for part in (hi, lo):
        spread_out = jnp.where(inside, part.astype(F32), 0.0).astype(BF)
        packed = packed + jnp.dot(spread_out, place, preferred_element_type=F32)
    k["rsc"][...] = packed.reshape(128, 1, 128)
    mine = sum(me[o] * STRIDE[o] for o in range(4))
    for t in spread(PEERS):
        there = sum(coord(o, t[o]) * STRIDE[o] for o in range(4))
        remote(k["rsc"].at[there], k["rr"].at[mine], k["s_ret"], k["r_ret"], t).start()
    k["rr"][mine] = k["rsc"][mine]
    k["hgs"][...] = (weight_row * k["acc"][...]).astype(BF)
    cp = pltpu.make_async_copy(k["hgs"], k["hg_h"], k["loc"].at[6])
    cp.start()
    out_cps[4] = cp
    weight_grad(0)
    few = k["rsc"].at[pl.ds(0, 127)]
    pltpu.make_async_copy(few, few, k["r_ret"]).wait()

    back = k["rr"][...].reshape(128, 128)
    mt = k["mt"][...]
    prob = k["prob"][...]
    score = jnp.zeros((128, 128), F32)
    for r in range(6):
        score = score + jnp.where(mt == float(r + 1), back[:, r : r + 1], 0.0)
    grad_t = prob * (score - jnp.sum(prob * score, 0, keepdims=True))
    grad = grad_t.T

    def halves(v):
        top = v.astype(BF)
        return top, (v - top.astype(F32)).astype(BF)

    hi, lo = halves(grad)
    xs = k["xs"]
    def router_rows(n):
        at = slice(1024 * n, min(D, 1024 * n + 1024))
        local = jnp.dot(k["normedt"][at, :], hi, preferred_element_type=F32) + jnp.dot(
            k["normedt"][at, :], lo, preferred_element_type=F32
        )
        blocks = (at.stop - at.start) // 8
        xs[pl.ds(128 * n, blocks)] = local.reshape(blocks, 8, 128).astype(BF)

    def send_color(n):
        a = COLORS[n][0]
        for d in (2, 1, 3):
            piece = xs.at[pl.ds(pl.multiple_of(128 * n + 32 * coord(a, d), 32), 32)]
            launch(piece, k["ar1"].at[n, d - 1], k["s_a1"].at[n], k["r_a1"].at[n], ring_offset(a, d))
        pending.append((k["ar1"].at[n], k["s_a1"].at[n]))

    for n in range(2):
        router_rows(n)
        send_color(n)
    router_rows(2)
    hi, lo = halves(grad_t)
    normed_grad = jnp.dot(k["rw"][...], hi, preferred_element_type=F32) + jnp.dot(
        k["rw"][...], lo, preferred_element_type=F32
    )
    floated = k["res"][...].astype(F32)
    inv = lax.rsqrt(jnp.mean(floated * floated, 0, keepdims=True) + 1e-05)
    unit = floated * inv
    gain_col = jnp.sum(normed_grad * unit, -1, keepdims=True)
    k["gv"][...] = jnp.zeros_like(k["gv"])
    for j in range(23):
        n = min(128, D - 128 * j)
        col = gain_col[128 * j : 128 * j + n]
        k["gv"][j : j + 1, 0:n] = jnp.sum(jnp.where(eye[:n, :n], col, 0.0), 0, keepdims=True)
    xs[pl.ds(360, 3)] = k["gv"][...].reshape(3, 8, 128).astype(BF)
    xs[pl.ds(363, 21)] = jnp.zeros((21, 8, 128), BF)
    send_color(2)
    upper = normed_grad * k["gc"][...]
    k["rg"][...] = (inv * (upper - unit * jnp.mean(upper * unit, 0, keepdims=True))).astype(BF)
    cp = pltpu.make_async_copy(k["rg"], k["rg_h"], k["loc"].at[12])
    cp.start()
    out_cps[5] = cp
    weight_grad(1)

    for n, (a, others) in enumerate(COLORS):
        wait_all(k["ar1"].at[n], k["r_a1"].at[n])
        total = xs[pl.ds(pl.multiple_of(128 * n + 32 * me[a], 32), 32)].astype(F32)
        for d in range(3):
            total = total + k["ar1"][n, d].astype(F32)
        k["as2"][n] = total.astype(BF)
        ring = (SZ[others[1]] * SZ[others[2]], SZ[others[2]], 1)

        def rank(t):
            return sum(coord(o, t[o]) * s for o, s in zip(others, ring))

        here = rank((0, 0, 0, 0))
        for t in spread(plane_offsets(others)):
            cp = remote(k["as2"].at[n, rank(t)], k["ar2"].at[n, here], k["s_a2"].at[n], k["r_a2"].at[n], t)
            cp.start()
        k["ar2"][n, here] = k["as2"][n, here]
    weight_grad(2)
    tot = k["tot"]
    for n, (a, others) in enumerate(COLORS):
        few = k["as2"].at[n, pl.ds(0, 31)]
        pltpu.make_async_copy(few, few, k["r_a2"].at[n]).wait()
        ring = (SZ[others[1]] * SZ[others[2]], SZ[others[2]], 1)
        here = sum(me[o] * s for o, s in zip(others, ring))
        done = jnp.sum(k["ar2"][n].astype(F32), 0)
        at = 128 * n + 32 * me[a] + here
        tot[at] = done.astype(BF)
        for t in spread(plane_offsets(others)):
            cp = remote(tot.at[at], tot.at[at], k["s_g2"].at[n], k["r_g2"].at[n], t)
            cp.start()
    weight_grad(3)
    for n, (a, others) in enumerate(COLORS):
        few = k["as2"].at[n, pl.ds(0, 31)]
        pltpu.make_async_copy(few, few, k["r_g2"].at[n]).wait()
        piece = tot.at[pl.ds(pl.multiple_of(128 * n + 32 * me[a], 32), 32)]
        for d in (2, 1, 3):
            launch(piece, piece, k["s_g1"].at[n], k["r_g1"].at[n], ring_offset(a, d))
        pending.append((tot.at[pl.ds(0, 96)], k["s_g1"].at[n]))
    for n in range(3):
        wait_all(tot.at[pl.ds(0, 96)], k["r_g1"].at[n])
        blocks = pl.ds(128 * n, 128)
        cp = pltpu.make_async_copy(k["tot"].at[blocks], k["tot_h"].at[blocks], k["loc"].at[13 + n])
        cp.start()
        out_cps[6 + n] = cp
    for ref, sem in pending:
        wait_all(ref, sem)
    few = k["rsc"].at[pl.ds(0, 127)]
    pltpu.make_async_copy(few, few, k["s_ret"]).wait()
    for n in range(3):
        few = k["as2"].at[n, pl.ds(0, 31)]
        pltpu.make_async_copy(few, few, k["s_a2"].at[n]).wait()
        pltpu.make_async_copy(few, few, k["s_g2"].at[n]).wait()
    for i, cp in out_cps.items():
        if i != 0:
            cp.wait()


def finish(hg, wg, rg, tot, hg_o, wg_o, rg_o, router, gain, hg_v, wg_v, rg_v, tot_v, ro_v, rsem, wsem):
    parts = [(tot, tot_v, None)]
    for src, via, dst, rows in ((wg, wg_v, wg_o, 240), (hg, hg_v, hg_o, 480), (rg, rg_v, rg_o, 1440)):
        for r in range(0, src.shape[0], rows):
            at = pl.ds(r, rows)
            parts.append((src.at[at], via.at[at], dst.at[at]))
    reads = [pltpu.make_async_copy(s, v, rsem.at[n]) for n, (s, v, d) in enumerate(parts)]
    for cp in reads:
        cp.start()
    writes = []
    for n, (s, v, d) in enumerate(parts):
        reads[n].wait()
        if d is None:
            ro_v[...] = tot_v[pl.ds(0, 360)].astype(F32).reshape(D, 128)
            cp = pltpu.make_async_copy(ro_v, router, wsem.at[n])
            cp.start()
            writes.append(cp)
            rows = tot_v[pl.ds(360, 3)].astype(F32).reshape(24, 128)
            for j in range(23):
                m = min(128, D - 128 * j)
                gain[pl.ds(128 * j, m)] = rows[j : j + 1, 0:m].reshape(m)
        else:
            cp = pltpu.make_async_copy(v, d, wsem.at[n])
            cp.start()
            writes.append(cp)
    for cp in writes:
        cp.wait()


def on_device(residual, norm_gain, router_weight, out_grad, expert_ids, hidden, down_weight):
    vm = pl.BlockSpec(memory_space=pltpu.VMEM)
    hbm = pl.BlockSpec(memory_space=pl.ANY)
    dma = pltpu.SemaphoreType.DMA
    scratch = [
        pltpu.VMEM((D, 128), BF), pltpu.VMEM((D, 128), BF), pltpu.VMEM((D,), F32), pltpu.VMEM((D, 128), BF),
        pltpu.VMEM((4, 128), jnp.int32), pltpu.VMEM((D, 128), BF), pltpu.VMEM((384, 8, 128), BF),
        pltpu.VMEM((FF, 768), BF), pltpu.VMEM((FF, D), BF), pltpu.VMEM((FF, 768), F32), pltpu.VMEM((FF, 768), BF),
        pltpu.VMEM((128, 128), F32), pltpu.VMEM((128, 128), F32), pltpu.VMEM((D, 128), BF), pltpu.VMEM((D, 128), F32),
        pltpu.VMEM((128, 1, 128), F32), pltpu.VMEM((128, 1, 128), F32),
        pltpu.VMEM((384, 8, 128), BF), pltpu.VMEM((3, 3, 32, 8, 128), BF), pltpu.VMEM((3, 32, 8, 128), BF),
        pltpu.VMEM((3, 32, 8, 128), BF), pltpu.VMEM((24, 128), F32), pltpu.VMEM((768, D), BF),
        pltpu.VMEM((FF, 768), BF), pltpu.VMEM((FF, 768), BF), pltpu.VMEM((FF, 576), BF),
        pltpu.VMEM((3, 3, 4, 128), jnp.int32),
    ]
    scratch += [pltpu.VMEM((4, 128, 128), BF) for _ in GDIMS]
    scratch += [pltpu.VMEM((4, 128, 128), BF)]
    scratch += [pltpu.VMEM((768, 512), BF) for _ in GDIMS]
    scratch += [pltpu.VMEM((768, 128), BF) for _ in GDIMS]
    scratch += [pltpu.VMEM((768, 768), BF) for _ in range(2)]
    for i, (c0, nc, cw, a, p, q) in enumerate(PLAN):
        sizes = tuple(SZ[o] for o in OTHER[a])
        scratch += [
            pltpu.VMEM((cw, 512), BF), pltpu.VMEM(sizes + (3, 8, cw), BF),
            pltpu.VMEM((4,) + tuple(SZ[o] for o in OTHER[a] if o != p) + (3, 8, cw), BF),
            pltpu.VMEM(sizes + (3, 8, cw), BF),
        ]
    scratch += [dma(()), dma((3,)), dma(()), dma(()), dma((NCH,)), dma((NCH, 2))]
    scratch += [dma((NCH,)), dma((NCH,)), dma((NCH,)), dma((NCH,))]
    scratch += [dma(()), dma(()), dma((3,)), dma((3,)), dma((3,)), dma((3,))]
    scratch += [dma((3,)), dma((3,)), dma((3,)), dma((3,)), dma((16,))]
    hidden_grad, weight_grad, residual_grad, total = pl.pallas_call(
        kernel,
        name="routed",
        out_shape=(
            jax.ShapeDtypeStruct((FF, 768), BF),
            jax.ShapeDtypeStruct((FF, D), BF),
            jax.ShapeDtypeStruct((D, 128), BF),
            jax.ShapeDtypeStruct((384, 8, 128), BF),
        ),
        in_specs=[hbm] * 7,
        out_specs=(hbm,) * 4,
        scratch_shapes=scratch,
        compiler_params=pltpu.CompilerParams(
            collective_id=0, has_side_effects=True, vmem_limit_bytes=67043328
        ),
    )(out_grad.T, residual.T, norm_gain, router_weight, expert_ids.T, hidden[0].T, down_weight[0])
    nparts = 1 + FF // 240 + FF // 480 + D // 1440
    hidden_grad, weight_grad, residual_grad, router_grad, gain_grad = pl.pallas_call(
        finish,
        name="finish",
        out_shape=(
            jax.ShapeDtypeStruct((FF, 768), BF),
            jax.ShapeDtypeStruct((FF, D), BF),
            jax.ShapeDtypeStruct((D, 128), BF),
            jax.ShapeDtypeStruct((D, 128), F32),
            jax.ShapeDtypeStruct((D,), F32),
        ),
        in_specs=[hbm, hbm, hbm, hbm],
        out_specs=(hbm, hbm, hbm, hbm, vm),
        scratch_shapes=[
            pltpu.VMEM((FF, 768), BF), pltpu.VMEM((FF, D), BF), pltpu.VMEM((D, 128), BF),
            pltpu.VMEM((384, 8, 128), BF), pltpu.VMEM((D, 128), F32), dma((nparts,)), dma((nparts,)),
        ],
        compiler_params=pltpu.CompilerParams(vmem_limit_bytes=67043328),
    )(hidden_grad, weight_grad, residual_grad, total)
    return hidden_grad.T[None], weight_grad[None], residual_grad.T, router_grad, gain_grad


def solution(mesh):
    finer = Mesh(mesh.devices.reshape(4, 4, 2, mesh.shape["dp"]), AX)
    rows = P(AX, None)
    cube = P(AX, None, None)
    return jax.shard_map(
        on_device,
        mesh=finer,
        in_specs=(rows, P(), P(), rows, rows, cube, cube),
        out_specs=(cube, cube, rows, P(), P()),
        check_vma=False,
    )
```
